128 devices in a mesh: src: 8 (over z, core), tile: 16 (over x, y).
Axes of the slice: x: 4, y: 4, z: 4, core: 2. Of those that a mesh axis runs over, the one named last changes fastest.
Arguments:
- tables: float32 [128, 32, 32, 1024], P(('src', 'tile')), may hold values from 0.2 to 2
- weights: float32 [128, 32], P(('src', 'tile')), may hold values from 0.05 to 0.5
- aperture: int32 [128, 32], P(('src', 'tile')), may hold values from 0 to 1, as said below
Outputs:
- image: float32 [32, 64, 32, 128], P('tile', 'src')
The draws below stay inside these ranges and needn't reach their ends.
Inputs may be any that keep to these rules, and one draw needn't show every extreme that they name: `aperture`: within one source and one group of 2 consecutive tiles (g * 2 to g * 2 + 1), at most 1 entries are 1; some group has exactly 1 for every source.
All inputs are finite; a program needn't handle non-finite values.
Results may differ from the reference program's by a relative error of at most 0.0003.
Values sent between devices are 32-bit elements; how exact they have to be, the bound alone decides.
A program may use at most 128 MiB of HBM per device.

```python
import math
import jax
import jax.numpy as jnp
from jax import lax

BX = 32
BY = 16
BZ = 64
BRICKS = 32
SOURCES = 128
GROUP = 2
CAP = 1


def draw_aperture(key, part):
    keys = jax.random.split(jax.random.fold_in(key, 17), 5)
    groups = BRICKS // GROUP
    heated = jax.random.randint(keys[0], (groups,), 0, 4) == 0
    filled_group = jax.random.randint(keys[1], (), 0, groups)
    group_ids = jnp.arange(groups)
    chance = jnp.where(heated, 85, 15)
    rolled = jax.random.randint(keys[2], (SOURCES, groups), 0, 100)
    partial_count = jax.random.randint(keys[3], (SOURCES, groups), 0, CAP)
    counts = jnp.where(rolled < chance[None, :], CAP, partial_count)
    counts = jnp.where(group_ids[None, :] == filled_group, CAP, counts)
    scores = jax.random.randint(keys[4], (SOURCES, groups, GROUP), 0, 1 << 20) * GROUP + jnp.arange(GROUP)
    ranking = jnp.sum((scores[:, :, None, :] < scores[:, :, :, None]).astype(jnp.int32), axis=3)
    chosen = ranking < counts[:, :, None]
    return chosen.reshape(SOURCES, BRICKS).astype(jnp.int32)


def level_of(rng, extent, cuts, smallest, largest):
    def one(dim, parts):
        draws = jax.random.uniform(jax.random.fold_in(jax.random.fold_in(rng, 6), dim), (parts,), jnp.float32, smallest / len(cuts), largest / len(cuts))
        return jnp.repeat(jnp.exp(draws), extent[dim] // parts).reshape((-1,) + (1,) * (len(extent) - dim - 1))

    gain = one(*cuts[0])
    for cut in cuts[1:]:
        gain = gain * one(*cut)
    return gain


def setup_inputs(seed: int = 0) -> dict:
    arg_keys = jax.random.split(jax.random.key(seed), 4)
    tables = jnp.clip(0.2 + 1.8 * jax.random.uniform(arg_keys[0], (SOURCES, BRICKS, BX, BY * BZ), jnp.float32) ** level_of(arg_keys[0], (SOURCES, BRICKS, BX, BY * BZ), ((0, 128),), -0.2, 0.2), 0.2, 2.0)
    weights = jnp.clip(jnp.exp(math.log(0.5) - 2.3025851 * jax.random.uniform(arg_keys[1], (SOURCES, BRICKS), jnp.float32) ** level_of(arg_keys[1], (SOURCES, BRICKS), ((0, 128),), -0.2, 0.2)), 0.05, 0.5)
    aperture = draw_aperture(jax.random.fold_in(arg_keys[3], 71), 0)
    return {"tables": tables, "weights": weights, "aperture": aperture}


angular_rate = 9.0


def refine_matrix(length):
    rows = jnp.arange(2 * length)
    cols = jnp.arange(length)
    center = rows // 2
    other = jnp.where(rows % 2 == 0, jnp.maximum(center - 1, 0), jnp.minimum(center + 1, length - 1))
    near = (cols[None, :] == center[:, None]).astype(jnp.float32)
    away = (cols[None, :] == other[:, None]).astype(jnp.float32)
    return 0.75 * near + 0.25 * away


def refine_all(bricks, rows_matrix, y_matrix, z_matrix):
    count = bricks.shape[0]
    fine_rows = rows_matrix.shape[0]
    along_x = jnp.einsum('fr,krc->kfc', rows_matrix, bricks, precision=lax.Precision.HIGHEST)
    flat = along_x.reshape(count * fine_rows * BY, BZ)
    along_z = jnp.dot(flat, z_matrix.T, precision=lax.Precision.HIGHEST).reshape(count, fine_rows, BY, 2 * BZ)
    return jnp.einsum('Yy,kfyz->kfYz', y_matrix, along_z, precision=lax.Precision.HIGHEST)


def reference(tables, weights, aperture):
    x_matrix = refine_matrix(BX)
    y_matrix = refine_matrix(BY)
    z_matrix = refine_matrix(BZ)
    scale = weights * aperture.astype(jnp.float32)

    def one_source(total, item):
        bricks, factor = item
        fine = refine_all(bricks, x_matrix, y_matrix, z_matrix)
        return total + factor[:, None, None, None] * jnp.cos(angular_rate * fine), None

    start = jnp.zeros((BRICKS, 2 * BX, 2 * BY, 2 * BZ), jnp.float32)
    total, unused = lax.scan(one_source, start, (tables, scale))
    return total
```

```python
import functools
import math

import jax
import jax.numpy as jnp
from jax import lax
from jax.experimental import pallas as pl
from jax.experimental.pallas import tpu as pltpu
from jax.sharding import PartitionSpec as P

BY = 16
BZ = 64
SUB = 8
LANES = 128
ROWS = 32
DEPTH = 16
COMPS = 4
PIECES = 2
KK = 4

angular_rate = 9.0
MESH = pl.DeviceIdType.MESH

CHUNKS = (
    (6, 0, 4),
    (4, 6, 0),
    (6, 10, 12),
    (2, 16, 10),
    (6, 18, 20),
    (2, 24, 18),
    (4, 26, 28),
    (2, 30, 26),
)


def sine_coefficients():
    import numpy as np

    n = 4
    k = np.arange(4000)
    r = 0.5 * np.cos((k + 0.5) * np.pi / 8000)
    powers = np.stack([r ** (2 * i + 1) for i in range(n)], axis=1)
    weight = 1.0 / np.sqrt(np.sin((k + 0.5) * np.pi / 8000) + 1e-3)
    target = np.sin(np.pi * r)
    for _ in range(60):
        got, *_rest = np.linalg.lstsq(powers * weight[:, None], target * weight, rcond=None)
        err = np.abs(powers @ got - target)
        weight = weight * (0.5 + 0.5 * err / err.max()) ** 0.5
        weight = weight / weight.max()
    return [float(np.float32(math.sqrt(2.0) * c)) for c in got]


def lane_masks(shape):
    lane = lax.broadcasted_iota(jnp.int32, shape, len(shape) - 1)
    sub = lax.broadcasted_iota(jnp.int32, shape, len(shape) - 2)
    z = lane & (BZ - 1)
    low = lane < BZ
    return z == 0, z == BZ - 1, low, low & (sub == 0), jnp.logical_not(low) & (sub == SUB - 1)


def kernel(
    coeffs,
    tables,
    weights,
    aperture,
    out,
    raw,
    send,
    recv,
    info_send,
    info_recv,
    splat,
    total_weight,
    fine,
    sib_send,
    sib_recv,
    far_send,
    far_recv,
    final,
    perm,
    load_sem,
    send_sem,
    recv_sem,
    info_ssem,
    info_rsem,
    sib_ssem,
    sib_rsem,
    far_ssem,
    far_rsem,
):
    a = lax.axis_index("src")
    t = lax.axis_index("tile")
    z, c = a // 2, a % 2
    tx, ty = t // 4, t % 4

    def owner_of(d):
        return ((tx + d // 4) % 4) * 4 + (ty + d % 4) % 4

    def load(i):
        first = pl.multiple_of(((z + 1 + i) % 4) * SUB, SUB)
        return pltpu.make_async_copy(
            tables.at[0, :, pl.ds(first, SUB), :], raw.at[i], load_sem.at[i]
        )

    for i in range(4):
        load(i).start()

    bar = pltpu.get_barrier_semaphore()

    def greet(d, carry):
        pl.semaphore_signal(bar, inc=1, device_id={"tile": owner_of(d), "src": a}, device_id_type=MESH)
        return carry

    lax.fori_loop(1, DEPTH, greet, 0)
    sibling = 2 * z + 1 - c
    pl.semaphore_signal(bar, inc=1, device_id={"src": sibling, "tile": t}, device_id_type=MESH)
    for m in range(3):
        far = 2 * ((z + 1 + m) % 4) + c
        pl.semaphore_signal(bar, inc=1, device_id={"src": far, "tile": t}, device_id_type=MESH)

    def fill_info(d, carry):
        first = 2 * owner_of(d)
        for j in range(2):
            w = jnp.full((SUB, LANES), weights[0, first + j], jnp.float32)
            live = jnp.full((SUB, LANES), aperture[0, first + j], jnp.int32)
            info_send[d, j] = w * live.astype(jnp.float32)
        return carry

    lax.fori_loop(0, DEPTH, fill_info, 0)

    def pick(i):
        def one(d, carry):
            first = 2 * owner_of(d)
            second = jnp.full((SUB, LANES), aperture[0, first + 1], jnp.int32) == 1
            for k in range(8):
                lanes = pl.ds(k * LANES, LANES)
                chosen = jnp.where(second, raw[i, first + 1, :, lanes], raw[i, first, :, lanes])
                send[d, pl.ds((1 + 8 * i) * SUB + k, SUB, stride=SUB), :] = chosen
            return carry

        lax.fori_loop(0, DEPTH, one, 0)

    load(0).wait()
    pick(0)
    load(3).wait()
    pick(3)

    def wrap(d, carry):
        send[d, pl.ds(0, SUB), :] = send[d, pl.ds(32 * SUB, SUB), :]
        return carry

    lax.fori_loop(0, DEPTH, wrap, 0)
    load(1).wait()
    pick(1)

    pl.semaphore_wait(bar, DEPTH - 1 + 4)

    def rows_of(n):
        size, start1, start0 = CHUNKS[n]
        start = start0 + (start1 - start0) * c
        return pl.ds(pl.multiple_of(start * SUB, SUB), size * SUB)

    def send_info(d, carry):
        pltpu.make_async_remote_copy(
            info_send.at[d], info_recv.at[d], info_ssem, info_rsem,
            device_id={"tile": owner_of(d), "src": a}, device_id_type=MESH,
        ).start()
        return carry

    def send_chunk(n):
        rows = rows_of(n)

        def one(d, carry):
            pltpu.make_async_remote_copy(
                send.at[d, rows], recv.at[d, rows], send_sem.at[n], recv_sem.at[n],
                device_id={"tile": owner_of(d), "src": a}, device_id_type=MESH,
            ).start()
            return carry

        lax.fori_loop(1, DEPTH, one, 0)

    def own_chunk(n):
        rows = rows_of(n)
        recv[0, rows, :] = send[0, rows, :]

    lax.fori_loop(1, DEPTH, send_info, 0)
    send_chunk(0)
    send_chunk(1)
    load(2).wait()
    pick(2)
    for n in range(2, 8):
        send_chunk(n)
    for n in range(8):
        own_chunk(n)

    row = lax.broadcasted_iota(jnp.int32, (2 * LANES, 2 * LANES), 0)
    col = lax.broadcasted_iota(jnp.int32, (2 * LANES, 2 * LANES), 1)
    place = ((row // BZ) % 2) * LANES + 2 * (row % BZ) + row // LANES
    perm[...] = (col == place).astype(jnp.float32).astype(jnp.bfloat16)

    info_send_bytes = info_send.at[pl.ds(1, DEPTH - 1)]
    pltpu.make_async_copy(
        info_send_bytes, info_recv.at[pl.ds(1, DEPTH - 1)], info_rsem
    ).wait()
    splat[0] = info_send[0]
    splat[pl.ds(1, DEPTH - 1)] = info_recv[pl.ds(1, DEPTH - 1)]
    total_weight[...] = jnp.sum(splat[...], axis=0)

    scale = angular_rate / (2.0 * math.pi) / 64.0
    group = 4

    def refine_rows(n):
        size, start1, start0 = CHUNKS[n]
        start = start0 + (start1 - start0) * c
        z_first, z_last, low, y_first, y_last = lane_masks((group, SUB, LANES))

        def one(i, carry):
            q = start + i // (DEPTH // group)
            s = (i % (DEPTH // group)) * group
            base = recv[pl.ds(s, group), pl.ds(pl.multiple_of(q * SUB, SUB), SUB), :] * scale
            triple = 3.0 * base
            below = jnp.where(z_first, base, pltpu.roll(base, 1, 2))
            above = jnp.where(z_last, base, pltpu.roll(base, LANES - 1, 2))
            for pz, v in enumerate((triple + below, triple + above)):
                swap = pltpu.roll(v, BZ, 2)
                down = pltpu.roll(swap, 1, 1)
                up = pltpu.roll(swap, SUB - 1, 1)
                before = jnp.where(y_first, v, jnp.where(low, down, swap))
                after = jnp.where(y_last, v, jnp.where(low, swap, up))
                v3 = 3.0 * v
                fine[q, pl.ds(s, group), pz] = v3 + before
                fine[q, pl.ds(s, group), 2 + pz] = v3 + after
            return carry

        lax.fori_loop(0, size * (DEPTH // group), one, 0)

    c0, c1, c2, c3 = coeffs

    def piece_rows(p):
        return pl.ds(p * (8 // PIECES), 8 // PIECES)

    def partial_rows(m, half, target, p):
        low_q = 8 * m + 4 * half
        owner = 2 * ((z + 1 + m) % 4) + half
        at_first = (owner == 0).astype(jnp.int32)
        at_last = (owner == 7).astype(jnp.int32)
        per = KK // PIECES

        def one_row(kk, carry):
            k = (low_q + 1 + kk) % ROWS
            prev = (low_q + kk + at_first * (kk == 0).astype(jnp.int32)) % ROWS
            following = (low_q + 2 + kk - at_last * (kk == KK - 1).astype(jnp.int32)) % ROWS

            def some_sources(g, acc):
                acc = list(acc)
                for u in range(2):
                    s = g * 2 + u
                    f0 = splat[s, 0]
                    f1 = splat[s, 1]
                    for comp in range(COMPS):
                        center = 3.0 * fine[k, s, comp]
                        for par, other in enumerate((prev, following)):
                            phase = center + fine[other, s, comp]
                            r = phase - lax.round(phase, lax.RoundingMethod.TO_NEAREST_EVEN)
                            sq = r * r
                            root = r * (((c3 * sq + c2) * sq + c1) * sq + c0)
                            val = root * root
                            at = par * 8 + comp
                            acc[at] = acc[at] + f0 * val
                            acc[at + 4] = acc[at + 4] + f1 * val
                return tuple(acc)

            zero = jnp.zeros((SUB, LANES), jnp.float32)
            acc = lax.fori_loop(0, DEPTH // 2, some_sources, (zero,) * 16)
            for par in range(2):
                for tile in range(2):
                    for comp in range(COMPS):
                        target[2 * kk + par, tile, comp] = (
                            total_weight[tile] - acc[par * 8 + tile * 4 + comp]
                        )
            return carry

        lax.fori_loop(p * per, (p + 1) * per, one_row, 0)

    def to_sibling(m, p):
        return pltpu.make_async_remote_copy(
            sib_send.at[m, piece_rows(p)], sib_recv.at[m, piece_rows(p)],
            sib_ssem.at[m, p], sib_rsem.at[m, p],
            device_id={"src": sibling, "tile": t}, device_id_type=MESH,
        )

    def to_owner(m, p):
        far = 2 * ((z + 1 + m) % 4) + c
        return pltpu.make_async_remote_copy(
            far_send.at[m, piece_rows(p)], far_recv.at[m, piece_rows(p)],
            far_ssem.at[m, p], far_rsem.at[m, p],
            device_id={"src": far, "tile": t}, device_id_type=MESH,
        )

    def wait_chunk(n):
        rows = rows_of(n)
        pltpu.make_async_copy(
            send.at[pl.ds(1, DEPTH - 1), rows], recv.at[pl.ds(1, DEPTH - 1), rows], recv_sem.at[n]
        ).wait()

    for m in range(4):
        wait_chunk(2 * m)
        refine_rows(2 * m)
        for p in range(PIECES):
            partial_rows(m, 1 - c, sib_send.at[m], p)
            to_sibling(m, p).start()
        wait_chunk(2 * m + 1)
        refine_rows(2 * m + 1)
        mine = far_send.at[m] if m < 3 else final
        for p in range(PIECES):
            partial_rows(m, c, mine, p)
            to_sibling(m, p).wait_recv()
            if m < 3:

                def add_sibling(x, carry):
                    far_send[m, x] = far_send[m, x] + sib_recv[m, x]
                    return carry

                lax.fori_loop(p * (8 // PIECES), (p + 1) * (8 // PIECES), add_sibling, 0)
                to_owner(m, p).start()

    for m in range(3):
        for p in range(PIECES):
            to_owner(m, p).wait_recv()

    for par in range(2):

        def finish(x, carry):
            for tile in range(2):
                for comp in range(2):
                    at = 2 * par + comp
                    got = final[x, tile, at] + sib_recv[3, x, tile, at]
                    for m in range(3):
                        got = got + far_recv[m, x, tile, at]
                    final[x, tile, at] = got
            return carry

        lax.fori_loop(0, 8, finish, 0)

    halves = [
        jnp.concatenate(
            [final[:, :, pl.ds(2 * par, 1)].reshape(16 * SUB, LANES),
             final[:, :, pl.ds(2 * par + 1, 1)].reshape(16 * SUB, LANES)], axis=1)
        for par in range(2)
    ]
    for par in range(2):
        value = halves[par]
        mixed = jnp.zeros((16 * SUB, 2 * LANES), jnp.float32)
        for _ in range(3):
            part = value.astype(jnp.bfloat16)
            value = value - part.astype(jnp.float32)
            mixed = mixed + jnp.dot(part, perm[...], preferred_element_type=jnp.float32)
        for x in range(8):
            for tile in range(2):
                at = (x * 2 + tile) * SUB
                for h in range(2):
                    out[tile, x, pl.ds(2 * h + par, SUB, stride=4), :] = (
                        mixed[at : at + SUB, h * LANES : (h + 1) * LANES]
                    )

    pltpu.make_async_copy(
        info_send_bytes, info_recv.at[pl.ds(1, DEPTH - 1)], info_ssem
    ).wait()
    for n in range(8):
        rows = rows_of(n)
        pltpu.make_async_copy(
            send.at[pl.ds(1, DEPTH - 1), rows], recv.at[pl.ds(1, DEPTH - 1), rows], send_sem.at[n]
        ).wait()
    for m in range(4):
        for p in range(PIECES):
            to_sibling(m, p).wait_send()
            if m < 3:
                to_owner(m, p).wait_send()


def shards(tables, weights, aperture):
    part = (8, 2, COMPS, SUB, LANES)
    vmem = pltpu.VMEM
    f32 = jnp.float32
    dma = pltpu.SemaphoreType.DMA
    return pl.pallas_call(
        functools.partial(kernel, sine_coefficients()),
        out_shape=jax.ShapeDtypeStruct((2, 8, 2 * BY, 2 * BZ), f32),
        in_specs=[
            pl.BlockSpec(memory_space=pl.ANY),
            pl.BlockSpec(memory_space=pltpu.SMEM),
            pl.BlockSpec(memory_space=pltpu.SMEM),
        ],
        out_specs=pl.BlockSpec(memory_space=pltpu.VMEM),
        scratch_shapes=[
            vmem((4, 32, SUB, 1024), f32),
            vmem((DEPTH, 33 * SUB, LANES), f32),
            vmem((DEPTH, ROWS * SUB, LANES), f32),
            vmem((DEPTH, 2, SUB, LANES), f32),
            vmem((DEPTH, 2, SUB, LANES), f32),
            vmem((DEPTH, 2, SUB, LANES), f32),
            vmem((2, SUB, LANES), f32),
            vmem((ROWS, DEPTH, COMPS, SUB, LANES), f32),
            vmem((4,) + part, f32),
            vmem((4,) + part, f32),
            vmem((3,) + part, f32),
            vmem((3,) + part, f32),
            vmem(part, f32),
            vmem((2 * LANES, 2 * LANES), jnp.bfloat16),
            dma((4,)),
            dma((8,)),
            dma((8,)),
            dma,
            dma,
            dma((4, PIECES)),
            dma((4, PIECES)),
            dma((3, PIECES)),
            dma((3, PIECES)),
        ],
        compiler_params=pltpu.CompilerParams(
            collective_id=0, has_side_effects=True, vmem_limit_bytes=60 * 2**20
        ),
    )(tables, weights, aperture)


def solution(mesh):
    placed = (
        P(("src", "tile"), None, None, None),
        P(("src", "tile"), None),
        P(("src", "tile"), None),
    )
    return jax.shard_map(
        shards, mesh=mesh, in_specs=placed, out_specs=P("tile", "src", None, None), check_vma=False
    )
```

```python
import functools
import math

import jax
import jax.numpy as jnp
from jax import lax
from jax.experimental import pallas as pl
from jax.experimental.pallas import tpu as pltpu
from jax.sharding import PartitionSpec as P

BY = 16
BZ = 64
SUB = 8
LANES = 128
ROWS = 32
DEPTH = 16
COMPS = 4
PIECES = 2
KK = 4

angular_rate = 9.0
MESH = pl.DeviceIdType.MESH

CHUNKS = (
    (6, 0, 4),
    (4, 6, 0),
    (6, 10, 12),
    (2, 16, 10),
    (6, 18, 20),
    (2, 24, 18),
    (4, 26, 28),
    (2, 30, 26),
)


def sine_coefficients():
    import numpy as np

    n = 4
    k = np.arange(4000)
    r = 0.5 * np.cos((k + 0.5) * np.pi / 8000)
    powers = np.stack([r ** (2 * i + 1) for i in range(n)], axis=1)
    weight = 1.0 / np.sqrt(np.sin((k + 0.5) * np.pi / 8000) + 1e-3)
    target = np.sin(np.pi * r)
    for _ in range(60):
        got, *_rest = np.linalg.lstsq(powers * weight[:, None], target * weight, rcond=None)
        err = np.abs(powers @ got - target)
        weight = weight * (0.5 + 0.5 * err / err.max()) ** 0.5
        weight = weight / weight.max()
    return [float(np.float32(math.sqrt(2.0) * c)) for c in got]


def lane_masks(shape):
    lane = lax.broadcasted_iota(jnp.int32, shape, len(shape) - 1)
    sub = lax.broadcasted_iota(jnp.int32, shape, len(shape) - 2)
    z = lane & (BZ - 1)
    low = lane < BZ
    return z == 0, z == BZ - 1, low, low & (sub == 0), jnp.logical_not(low) & (sub == SUB - 1)


def kernel(
    coeffs,
    tables,
    weights,
    aperture,
    out,
    raw,
    send,
    recv,
    info_send,
    info_recv,
    splat,
    total_weight,
    fine,
    sib_send,
    sib_recv,
    far_send,
    far_recv,
    final,
    perm,
    load_sem,
    send_sem,
    recv_sem,
    info_ssem,
    info_rsem,
    sib_ssem,
    sib_rsem,
    far_ssem,
    far_rsem,
):
    a = lax.axis_index("src")
    t = lax.axis_index("tile")
    z, c = a // 2, a % 2
    tx, ty = t // 4, t % 4

    def owner_of(d):
        return ((tx + d // 4) % 4) * 4 + (ty + d % 4) % 4

    def load(i):
        first = pl.multiple_of(((z + 1 + i) % 4) * SUB, SUB)
        return pltpu.make_async_copy(
            tables.at[0, :, pl.ds(first, SUB), :], raw.at[i], load_sem.at[i]
        )

    for i in range(4):
        load(i).start()

    bar = pltpu.get_barrier_semaphore()

    def greet(d, carry):
        pl.semaphore_signal(bar, inc=1, device_id={"tile": owner_of(d), "src": a}, device_id_type=MESH)
        return carry

    lax.fori_loop(1, DEPTH, greet, 0)
    sibling = 2 * z + 1 - c
    pl.semaphore_signal(bar, inc=1, device_id={"src": sibling, "tile": t}, device_id_type=MESH)
    for m in range(3):
        far = 2 * ((z + 1 + m) % 4) + c
        pl.semaphore_signal(bar, inc=1, device_id={"src": far, "tile": t}, device_id_type=MESH)

    def fill_info(d, carry):
        first = 2 * owner_of(d)
        for j in range(2):
            w = jnp.full((SUB, LANES), weights[0, first + j], jnp.float32)
            live = jnp.full((SUB, LANES), aperture[0, first + j], jnp.int32)
            info_send[d, j] = w * live.astype(jnp.float32)
        return carry

    lax.fori_loop(0, DEPTH, fill_info, 0)

    scale = angular_rate / (2.0 * math.pi) / 64.0

    def pick(i):
        def one(d, carry):
            first = 2 * owner_of(d)
            second = jnp.full((SUB, LANES), aperture[0, first + 1], jnp.int32) == 1
            for k in range(8):
                lanes = pl.ds(k * LANES, LANES)
                chosen = jnp.where(second, raw[i, first + 1, :, lanes], raw[i, first, :, lanes])
                send[d, pl.ds((1 + 8 * i) * SUB + k, SUB, stride=SUB), :] = chosen * scale
            return carry

        lax.fori_loop(0, DEPTH, one, 0)

    load(0).wait()
    pick(0)
    load(3).wait()
    pick(3)

    def wrap(d, carry):
        send[d, pl.ds(0, SUB), :] = send[d, pl.ds(32 * SUB, SUB), :]
        return carry

    lax.fori_loop(0, DEPTH, wrap, 0)
    load(1).wait()
    pick(1)

    pl.semaphore_wait(bar, DEPTH - 1 + 4)

    def rows_of(n):
        size, start1, start0 = CHUNKS[n]
        start = start0 + (start1 - start0) * c
        return pl.ds(pl.multiple_of(start * SUB, SUB), size * SUB)

    def send_info(d, carry):
        pltpu.make_async_remote_copy(
            info_send.at[d], info_recv.at[d], info_ssem, info_rsem,
            device_id={"tile": owner_of(d), "src": a}, device_id_type=MESH,
        ).start()
        return carry

    def send_chunk(n):
        rows = rows_of(n)

        def one(d, carry):
            pltpu.make_async_remote_copy(
                send.at[d, rows], recv.at[d, rows], send_sem.at[n], recv_sem.at[n],
                device_id={"tile": owner_of(d), "src": a}, device_id_type=MESH,
            ).start()
            return carry

        lax.fori_loop(1, DEPTH, one, 0)

    def own_chunk(n):
        rows = rows_of(n)
        recv[0, rows, :] = send[0, rows, :]

    lax.fori_loop(1, DEPTH, send_info, 0)
    send_chunk(0)
    send_chunk(1)
    load(2).wait()
    pick(2)
    for n in range(2, 8):
        send_chunk(n)
    for n in range(8):
        own_chunk(n)

    row = lax.broadcasted_iota(jnp.int32, (2 * LANES, 2 * LANES), 0)
    col = lax.broadcasted_iota(jnp.int32, (2 * LANES, 2 * LANES), 1)
    place = ((row // BZ) % 2) * LANES + 2 * (row % BZ) + row // LANES
    perm[...] = (col == place).astype(jnp.float32).astype(jnp.bfloat16)

    info_send_bytes = info_send.at[pl.ds(1, DEPTH - 1)]
    pltpu.make_async_copy(
        info_send_bytes, info_recv.at[pl.ds(1, DEPTH - 1)], info_rsem
    ).wait()
    splat[0] = info_send[0]
    splat[pl.ds(1, DEPTH - 1)] = info_recv[pl.ds(1, DEPTH - 1)]
    total_weight[...] = jnp.sum(splat[...], axis=0)

    def refine_rows(n):
        size, start1, start0 = CHUNKS[n]
        start = start0 + (start1 - start0) * c
        z_first, z_last, low, y_first, y_last = lane_masks((SUB, LANES))

        def one(i, carry):
            q = start + i
            for s in range(DEPTH):
                base = recv[s, pl.ds(pl.multiple_of(q * SUB, SUB), SUB), :]
                swap = pltpu.roll(base, BZ, 1)
                below = jnp.where(z_first, base, pltpu.roll(base, 1, 1))
                above = jnp.where(z_last, base, pltpu.roll(base, LANES - 1, 1))
                swap_below = jnp.where(z_first, swap, pltpu.roll(base, BZ + 1, 1))
                swap_above = jnp.where(z_last, swap, pltpu.roll(base, BZ - 1, 1))
                triple = 3.0 * base
                swap_triple = 3.0 * swap
                for pz in range(2):
                    v = triple + (above if pz else below)
                    w = swap_triple + (swap_above if pz else swap_below)
                    down = pltpu.roll(w, 1, 0)
                    up = pltpu.roll(w, SUB - 1, 0)
                    before = jnp.where(y_first, v, jnp.where(low, down, w))
                    after = jnp.where(y_last, v, jnp.where(low, w, up))
                    v3 = 3.0 * v
                    fine[q, s, pz] = v3 + before
                    fine[q, s, 2 + pz] = v3 + after
            return carry

        lax.fori_loop(0, size, one, 0)

    c0, c1, c2, c3 = coeffs

    def piece_rows(p):
        return pl.ds(p * (8 // PIECES), 8 // PIECES)

    def partial_rows(m, half, target, p):
        low_q = 8 * m + 4 * half
        owner = 2 * ((z + 1 + m) % 4) + half
        at_first = (owner == 0).astype(jnp.int32)
        at_last = (owner == 7).astype(jnp.int32)
        per = KK // PIECES

        def one_row(kk, carry):
            k = (low_q + 1 + kk) % ROWS
            prev = (low_q + kk + at_first * (kk == 0).astype(jnp.int32)) % ROWS
            following = (low_q + 2 + kk - at_last * (kk == KK - 1).astype(jnp.int32)) % ROWS

            def some_sources(g, acc):
                acc = list(acc)
                for u in range(4):
                    s = g * 4 + u
                    f0 = splat[s, 0]
                    f1 = splat[s, 1]
                    for comp in range(COMPS):
                        center = 3.0 * fine[k, s, comp]
                        for par, other in enumerate((prev, following)):
                            phase = center + fine[other, s, comp]
                            r = phase - lax.round(phase, lax.RoundingMethod.TO_NEAREST_EVEN)
                            sq = r * r
                            root = r * (((c3 * sq + c2) * sq + c1) * sq + c0)
                            val = root * root
                            at = par * 8 + comp
                            acc[at] = acc[at] + f0 * val
                            acc[at + 4] = acc[at + 4] + f1 * val
                return tuple(acc)

            zero = jnp.zeros((SUB, LANES), jnp.float32)
            acc = lax.fori_loop(0, DEPTH // 4, some_sources, (zero,) * 16)
            for par in range(2):
                for tile in range(2):
                    for comp in range(COMPS):
                        target[2 * kk + par, tile, comp] = (
                            total_weight[tile] - acc[par * 8 + tile * 4 + comp]
                        )
            return carry

        lax.fori_loop(p * per, (p + 1) * per, one_row, 0)

    def to_sibling(m, p):
        return pltpu.make_async_remote_copy(
            sib_send.at[m, piece_rows(p)], sib_recv.at[m, piece_rows(p)],
            sib_ssem.at[m, p], sib_rsem.at[m, p],
            device_id={"src": sibling, "tile": t}, device_id_type=MESH,
        )

    def to_owner(m, p):
        far = 2 * ((z + 1 + m) % 4) + c
        return pltpu.make_async_remote_copy(
            far_send.at[m, piece_rows(p)], far_recv.at[m, piece_rows(p)],
            far_ssem.at[m, p], far_rsem.at[m, p],
            device_id={"src": far, "tile": t}, device_id_type=MESH,
        )

    def wait_chunk(n):
        rows = rows_of(n)
        pltpu.make_async_copy(
            send.at[pl.ds(1, DEPTH - 1), rows], recv.at[pl.ds(1, DEPTH - 1), rows], recv_sem.at[n]
        ).wait()

    for m in range(4):
        wait_chunk(2 * m)
        refine_rows(2 * m)
        for p in range(PIECES):
            partial_rows(m, 1 - c, sib_send.at[m], p)
            to_sibling(m, p).start()
        wait_chunk(2 * m + 1)
        refine_rows(2 * m + 1)
        mine = far_send.at[m] if m < 3 else final
        for p in range(PIECES):
            partial_rows(m, c, mine, p)
            to_sibling(m, p).wait_recv()
            if m < 3:

                def add_sibling(x, carry):
                    far_send[m, x] = far_send[m, x] + sib_recv[m, x]
                    return carry

                lax.fori_loop(p * (8 // PIECES), (p + 1) * (8 // PIECES), add_sibling, 0)
                to_owner(m, p).start()

    for m in range(3):
        for p in range(PIECES):
            to_owner(m, p).wait_recv()

    for par in range(2):

        def finish(x, carry):
            for tile in range(2):
                for comp in range(2):
                    at = 2 * par + comp
                    got = final[x, tile, at] + sib_recv[3, x, tile, at]
                    for m in range(3):
                        got = got + far_recv[m, x, tile, at]
                    final[x, tile, at] = got
            return carry

        lax.fori_loop(0, 8, finish, 0)

    halves = [
        jnp.concatenate(
            [final[:, :, pl.ds(2 * par, 1)].reshape(16 * SUB, LANES),
             final[:, :, pl.ds(2 * par + 1, 1)].reshape(16 * SUB, LANES)], axis=1)
        for par in range(2)
    ]
    for par in range(2):
        value = halves[par]
        mixed = jnp.zeros((16 * SUB, 2 * LANES), jnp.float32)
        for _ in range(3):
            part = value.astype(jnp.bfloat16)
            value = value - part.astype(jnp.float32)
            mixed = mixed + jnp.dot(part, perm[...], preferred_element_type=jnp.float32)
        for x in range(8):
            for tile in range(2):
                at = (x * 2 + tile) * SUB
                for h in range(2):
                    out[tile, x, pl.ds(2 * h + par, SUB, stride=4), :] = (
                        mixed[at : at + SUB, h * LANES : (h + 1) * LANES]
                    )

    pltpu.make_async_copy(
        info_send_bytes, info_recv.at[pl.ds(1, DEPTH - 1)], info_ssem
    ).wait()
    for n in range(8):
        rows = rows_of(n)
        pltpu.make_async_copy(
            send.at[pl.ds(1, DEPTH - 1), rows], recv.at[pl.ds(1, DEPTH - 1), rows], send_sem.at[n]
        ).wait()
    for m in range(4):
        for p in range(PIECES):
            to_sibling(m, p).wait_send()
            if m < 3:
                to_owner(m, p).wait_send()


def shards(tables, weights, aperture):
    part = (8, 2, COMPS, SUB, LANES)
    vmem = pltpu.VMEM
    f32 = jnp.float32
    dma = pltpu.SemaphoreType.DMA
    return pl.pallas_call(
        functools.partial(kernel, sine_coefficients()),
        out_shape=jax.ShapeDtypeStruct((2, 8, 2 * BY, 2 * BZ), f32),
        in_specs=[
            pl.BlockSpec(memory_space=pl.ANY),
            pl.BlockSpec(memory_space=pltpu.SMEM),
            pl.BlockSpec(memory_space=pltpu.SMEM),
        ],
        out_specs=pl.BlockSpec(memory_space=pltpu.VMEM),
        scratch_shapes=[
            vmem((4, 32, SUB, 1024), f32),
            vmem((DEPTH, 33 * SUB, LANES), f32),
            vmem((DEPTH, ROWS * SUB, LANES), f32),
            vmem((DEPTH, 2, SUB, LANES), f32),
            vmem((DEPTH, 2, SUB, LANES), f32),
            vmem((DEPTH, 2, SUB, LANES), f32),
            vmem((2, SUB, LANES), f32),
            vmem((ROWS, DEPTH, COMPS, SUB, LANES), f32),
            vmem((4,) + part, f32),
            vmem((4,) + part, f32),
            vmem((3,) + part, f32),
            vmem((3,) + part, f32),
            vmem(part, f32),
            vmem((2 * LANES, 2 * LANES), jnp.bfloat16),
            dma((4,)),
            dma((8,)),
            dma((8,)),
            dma,
            dma,
            dma((4, PIECES)),
            dma((4, PIECES)),
            dma((3, PIECES)),
            dma((3, PIECES)),
        ],
        compiler_params=pltpu.CompilerParams(
            collective_id=0, has_side_effects=True, vmem_limit_bytes=60 * 2**20
        ),
    )(tables, weights, aperture)


def solution(mesh):
    placed = (
        P(("src", "tile"), None, None, None),
        P(("src", "tile"), None),
        P(("src", "tile"), None),
    )
    return jax.shard_map(
        shards, mesh=mesh, in_specs=placed, out_specs=P("tile", "src", None, None), check_vma=False
    )
```

```python
import functools
import math

import jax
import jax.numpy as jnp
from jax import lax
from jax.experimental import pallas as pl
from jax.experimental.pallas import tpu as pltpu
from jax.sharding import PartitionSpec as P

BY = 16
BZ = 64
SUB = 8
LANES = 128
ROWS = 32
DEPTH = 16
COMPS = 4
PIECES = 2
KK = 4

angular_rate = 9.0
MESH = pl.DeviceIdType.MESH

CHUNKS = (
    (6, 8, 12),
    (4, 14, 8),
    (4, 18, 4),
    (4, 4, 18),
    (4, 0, 22),
    (4, 22, 0),
    (4, 26, 28),
    (2, 30, 26),
)
GROUPS = (
    ((2, 1), (2, 0)),
    ((1, 1), (3, 0)),
    ((3, 1), (1, 0)),
    ((4, 1), (4, 0)),
)


def sine_coefficients():
    import numpy as np

    n = 4
    k = np.arange(4000)
    r = 0.5 * np.cos((k + 0.5) * np.pi / 8000)
    powers = np.stack([r ** (2 * i + 1) for i in range(n)], axis=1)
    weight = 1.0 / np.sqrt(np.sin((k + 0.5) * np.pi / 8000) + 1e-3)
    target = np.sin(np.pi * r)
    for _ in range(60):
        got, *_rest = np.linalg.lstsq(powers * weight[:, None], target * weight, rcond=None)
        err = np.abs(powers @ got - target)
        weight = weight * (0.5 + 0.5 * err / err.max()) ** 0.5
        weight = weight / weight.max()
    return [float(np.float32(math.sqrt(2.0) * c)) for c in got]


def lane_masks(shape):
    lane = lax.broadcasted_iota(jnp.int32, shape, len(shape) - 1)
    sub = lax.broadcasted_iota(jnp.int32, shape, len(shape) - 2)
    z = lane & (BZ - 1)
    low = lane < BZ
    return z == 0, z == BZ - 1, low, low & (sub == 0), jnp.logical_not(low) & (sub == SUB - 1)


def kernel(
    coeffs,
    tables,
    weights,
    aperture,
    out,
    raw,
    send,
    recv,
    info_send,
    info_recv,
    splat,
    total_weight,
    fine,
    sib_send,
    sib_recv,
    far_send,
    far_recv,
    final,
    perm,
    load_sem,
    send_sem,
    recv_sem,
    info_ssem,
    info_rsem,
    sib_ssem,
    sib_rsem,
    far_ssem,
    far_rsem,
):
    a = lax.axis_index("src")
    t = lax.axis_index("tile")
    z, c = a // 2, a % 2
    tx, ty = t // 4, t % 4

    def owner_of(d):
        return ((tx + d // 4) % 4) * 4 + (ty + d % 4) % 4

    def load(i):
        first = pl.multiple_of(((z + 1 + i) % 4) * SUB, SUB)
        return pltpu.make_async_copy(
            tables.at[0, :, pl.ds(first, SUB), :], raw.at[i], load_sem.at[i]
        )

    for i in (1, 0, 2, 3):
        load(i).start()

    bar = pltpu.get_barrier_semaphore()

    def greet(d, carry):
        pl.semaphore_signal(bar, inc=1, device_id={"tile": owner_of(d), "src": a}, device_id_type=MESH)
        return carry

    lax.fori_loop(1, DEPTH, greet, 0)
    sibling = 2 * z + 1 - c
    pl.semaphore_signal(bar, inc=1, device_id={"src": sibling, "tile": t}, device_id_type=MESH)
    for m in range(3):
        far = 2 * ((z + 1 + m) % 4) + c
        pl.semaphore_signal(bar, inc=1, device_id={"src": far, "tile": t}, device_id_type=MESH)

    def fill_info(d, carry):
        first = 2 * owner_of(d)
        for j in range(2):
            w = jnp.full((SUB, LANES), weights[0, first + j], jnp.float32)
            live = jnp.full((SUB, LANES), aperture[0, first + j], jnp.int32)
            info_send[d, j] = w * live.astype(jnp.float32)
        return carry

    lax.fori_loop(0, DEPTH, fill_info, 0)

    scale = angular_rate / (2.0 * math.pi) / 64.0

    def pick(i):
        def one(d, carry):
            first = 2 * owner_of(d)
            second = jnp.full((SUB, LANES), aperture[0, first + 1], jnp.int32) == 1
            for k in range(8):
                lanes = pl.ds(k * LANES, LANES)
                chosen = jnp.where(second, raw[i, first + 1, :, lanes], raw[i, first, :, lanes])
                send[d, pl.ds((1 + 8 * i) * SUB + k, SUB, stride=SUB), :] = chosen * scale
            return carry

        lax.fori_loop(0, DEPTH, one, 0)

    for i in (1, 0, 2):
        load(i).wait()
        pick(i)

    pl.semaphore_wait(bar, DEPTH - 1 + 4)

    def rows_of(n):
        size, start1, start0 = CHUNKS[n]
        start = start0 + (start1 - start0) * c
        return pl.ds(pl.multiple_of(start * SUB, SUB), size * SUB)

    def send_info(d, carry):
        pltpu.make_async_remote_copy(
            info_send.at[d], info_recv.at[d], info_ssem, info_rsem,
            device_id={"tile": owner_of(d), "src": a}, device_id_type=MESH,
        ).start()
        return carry

    def send_chunk(n):
        rows = rows_of(n)

        def one(d, carry):
            pltpu.make_async_remote_copy(
                send.at[d, rows], recv.at[d, rows], send_sem.at[n], recv_sem.at[n],
                device_id={"tile": owner_of(d), "src": a}, device_id_type=MESH,
            ).start()
            return carry

        lax.fori_loop(1, DEPTH, one, 0)

    def own_chunk(n):
        rows = rows_of(n)
        recv[0, rows, :] = send[0, rows, :]

    lax.fori_loop(1, DEPTH, send_info, 0)
    for n in range(4):
        send_chunk(n)
    load(3).wait()
    pick(3)

    def wrap(d, carry):
        send[d, pl.ds(0, SUB), :] = send[d, pl.ds(32 * SUB, SUB), :]
        return carry

    lax.fori_loop(0, DEPTH, wrap, 0)
    for n in range(4, 8):
        send_chunk(n)
    for n in range(8):
        own_chunk(n)

    row = lax.broadcasted_iota(jnp.int32, (2 * LANES, 2 * LANES), 0)
    col = lax.broadcasted_iota(jnp.int32, (2 * LANES, 2 * LANES), 1)
    place = ((row // BZ) % 2) * LANES + 2 * (row % BZ) + row // LANES
    perm[...] = (col == place).astype(jnp.float32).astype(jnp.bfloat16)

    info_send_bytes = info_send.at[pl.ds(1, DEPTH - 1)]
    pltpu.make_async_copy(
        info_send_bytes, info_recv.at[pl.ds(1, DEPTH - 1)], info_rsem
    ).wait()
    splat[0] = info_send[0]
    splat[pl.ds(1, DEPTH - 1)] = info_recv[pl.ds(1, DEPTH - 1)]
    total_weight[...] = jnp.sum(splat[...], axis=0)

    def refine_rows(n):
        size, start1, start0 = CHUNKS[n]
        start = start0 + (start1 - start0) * c
        z_first, z_last, low, y_first, y_last = lane_masks((SUB, LANES))

        def one(i, carry):
            q = start + i
            for s in range(DEPTH):
                base = recv[s, pl.ds(pl.multiple_of(q * SUB, SUB), SUB), :]
                swap = pltpu.roll(base, BZ, 1)
                below = jnp.where(z_first, base, pltpu.roll(base, 1, 1))
                above = jnp.where(z_last, base, pltpu.roll(base, LANES - 1, 1))
                swap_below = jnp.where(z_first, swap, pltpu.roll(base, BZ + 1, 1))
                swap_above = jnp.where(z_last, swap, pltpu.roll(base, BZ - 1, 1))
                triple = 3.0 * base
                swap_triple = 3.0 * swap
                for pz in range(2):
                    v = triple + (above if pz else below)
                    w = swap_triple + (swap_above if pz else swap_below)
                    down = pltpu.roll(w, 1, 0)
                    up = pltpu.roll(w, SUB - 1, 0)
                    before = jnp.where(y_first, v, jnp.where(low, down, w))
                    after = jnp.where(y_last, v, jnp.where(low, w, up))
                    v3 = 3.0 * v
                    fine[q, s, pz] = v3 + before
                    fine[q, s, 2 + pz] = v3 + after
            return carry

        lax.fori_loop(0, size, one, 0)

    c0, c1, c2, c3 = coeffs

    def owner_place(m, who):
        (ahead1, half1), (ahead0, half0) = GROUPS[m]
        return ahead0 + (ahead1 - ahead0) * who, half0 + (half1 - half0) * who

    def piece_rows(p):
        return pl.ds(p * (8 // PIECES), 8 // PIECES)

    def partial_rows(m, who, target, p):
        ahead, half = owner_place(m, who)
        low_q = 8 * (ahead - 1) + 4 * half
        owner = 2 * ((z + ahead) % 4) + half
        at_first = (owner == 0).astype(jnp.int32)
        at_last = (owner == 7).astype(jnp.int32)
        per = KK // PIECES

        def one_row(kk, carry):
            k = (low_q + 1 + kk) % ROWS
            prev = (low_q + kk + at_first * (kk == 0).astype(jnp.int32)) % ROWS
            following = (low_q + 2 + kk - at_last * (kk == KK - 1).astype(jnp.int32)) % ROWS

            def some_sources(g, acc):
                acc = list(acc)
                for u in range(4):
                    s = g * 4 + u
                    f0 = splat[s, 0]
                    f1 = splat[s, 1]
                    for comp in range(COMPS):
                        center = 3.0 * fine[k, s, comp]
                        for par, other in enumerate((prev, following)):
                            phase = center + fine[other, s, comp]
                            r = phase - lax.round(phase, lax.RoundingMethod.TO_NEAREST_EVEN)
                            sq = r * r
                            root = r * (((c3 * sq + c2) * sq + c1) * sq + c0)
                            val = root * root
                            at = par * 8 + comp
                            acc[at] = acc[at] + f0 * val
                            acc[at + 4] = acc[at + 4] + f1 * val
                return tuple(acc)

            zero = jnp.zeros((SUB, LANES), jnp.float32)
            acc = lax.fori_loop(0, DEPTH // 4, some_sources, (zero,) * 16)
            for par in range(2):
                for tile in range(2):
                    for comp in range(COMPS):
                        target[2 * kk + par, tile, comp] = (
                            total_weight[tile] - acc[par * 8 + tile * 4 + comp]
                        )
            return carry

        lax.fori_loop(p * per, (p + 1) * per, one_row, 0)

    def to_sibling(m, p):
        return pltpu.make_async_remote_copy(
            sib_send.at[m, piece_rows(p)], sib_recv.at[m, piece_rows(p)],
            sib_ssem.at[m, p], sib_rsem.at[m, p],
            device_id={"src": sibling, "tile": t}, device_id_type=MESH,
        )

    def to_owner(m, p):
        ahead, half = owner_place(m, c)
        far = 2 * ((z + ahead) % 4) + half
        return pltpu.make_async_remote_copy(
            far_send.at[m, piece_rows(p)], far_recv.at[m, piece_rows(p)],
            far_ssem.at[m, p], far_rsem.at[m, p],
            device_id={"src": far, "tile": t}, device_id_type=MESH,
        )

    def wait_chunk(n):
        rows = rows_of(n)
        pltpu.make_async_copy(
            send.at[pl.ds(1, DEPTH - 1), rows], recv.at[pl.ds(1, DEPTH - 1), rows], recv_sem.at[n]
        ).wait()

    for m in range(4):
        wait_chunk(2 * m)
        refine_rows(2 * m)
        for p in range(PIECES):
            partial_rows(m, 1 - c, sib_send.at[m], p)
            to_sibling(m, p).start()
        wait_chunk(2 * m + 1)
        refine_rows(2 * m + 1)
        mine = far_send.at[m] if m < 3 else final
        for p in range(PIECES):
            partial_rows(m, c, mine, p)
            to_sibling(m, p).wait_recv()
            if m < 3:

                def add_sibling(x, carry):
                    far_send[m, x] = far_send[m, x] + sib_recv[m, x]
                    return carry

                lax.fori_loop(p * (8 // PIECES), (p + 1) * (8 // PIECES), add_sibling, 0)
                to_owner(m, p).start()

    for m in range(3):
        for p in range(PIECES):
            to_owner(m, p).wait_recv()

    for par in range(2):

        def finish(x, carry):
            for tile in range(2):
                for comp in range(2):
                    at = 2 * par + comp
                    got = final[x, tile, at] + sib_recv[3, x, tile, at]
                    for m in range(3):
                        got = got + far_recv[m, x, tile, at]
                    final[x, tile, at] = got
            return carry

        lax.fori_loop(0, 8, finish, 0)

    halves = [
        jnp.concatenate(
            [final[:, :, pl.ds(2 * par, 1)].reshape(16 * SUB, LANES),
             final[:, :, pl.ds(2 * par + 1, 1)].reshape(16 * SUB, LANES)], axis=1)
        for par in range(2)
    ]
    for par in range(2):
        value = halves[par]
        mixed = jnp.zeros((16 * SUB, 2 * LANES), jnp.float32)
        for _ in range(3):
            part = value.astype(jnp.bfloat16)
            value = value - part.astype(jnp.float32)
            mixed = mixed + jnp.dot(part, perm[...], preferred_element_type=jnp.float32)
        for x in range(8):
            for tile in range(2):
                at = (x * 2 + tile) * SUB
                for h in range(2):
                    out[tile, x, pl.ds(2 * h + par, SUB, stride=4), :] = (
                        mixed[at : at + SUB, h * LANES : (h + 1) * LANES]
                    )

    pltpu.make_async_copy(
        info_send_bytes, info_recv.at[pl.ds(1, DEPTH - 1)], info_ssem
    ).wait()
    for n in range(8):
        rows = rows_of(n)
        pltpu.make_async_copy(
            send.at[pl.ds(1, DEPTH - 1), rows], recv.at[pl.ds(1, DEPTH - 1), rows], send_sem.at[n]
        ).wait()
    for m in range(4):
        for p in range(PIECES):
            to_sibling(m, p).wait_send()
            if m < 3:
                to_owner(m, p).wait_send()


def shards(tables, weights, aperture):
    part = (8, 2, COMPS, SUB, LANES)
    vmem = pltpu.VMEM
    f32 = jnp.float32
    dma = pltpu.SemaphoreType.DMA
    return pl.pallas_call(
        functools.partial(kernel, sine_coefficients()),
        out_shape=jax.ShapeDtypeStruct((2, 8, 2 * BY, 2 * BZ), f32),
        in_specs=[
            pl.BlockSpec(memory_space=pl.ANY),
            pl.BlockSpec(memory_space=pltpu.SMEM),
            pl.BlockSpec(memory_space=pltpu.SMEM),
        ],
        out_specs=pl.BlockSpec(memory_space=pltpu.VMEM),
        scratch_shapes=[
            vmem((4, 32, SUB, 1024), f32),
            vmem((DEPTH, 33 * SUB, LANES), f32),
            vmem((DEPTH, ROWS * SUB, LANES), f32),
            vmem((DEPTH, 2, SUB, LANES), f32),
            vmem((DEPTH, 2, SUB, LANES), f32),
            vmem((DEPTH, 2, SUB, LANES), f32),
            vmem((2, SUB, LANES), f32),
            vmem((ROWS, DEPTH, COMPS, SUB, LANES), f32),
            vmem((4,) + part, f32),
            vmem((4,) + part, f32),
            vmem((3,) + part, f32),
            vmem((3,) + part, f32),
            vmem(part, f32),
            vmem((2 * LANES, 2 * LANES), jnp.bfloat16),
            dma((4,)),
            dma((8,)),
            dma((8,)),
            dma,
            dma,
            dma((4, PIECES)),
            dma((4, PIECES)),
            dma((3, PIECES)),
            dma((3, PIECES)),
        ],
        compiler_params=pltpu.CompilerParams(
            collective_id=0, has_side_effects=True, vmem_limit_bytes=60 * 2**20
        ),
    )(tables, weights, aperture)


def solution(mesh):
    placed = (
        P(("src", "tile"), None, None, None),
        P(("src", "tile"), None),
        P(("src", "tile"), None),
    )
    return jax.shard_map(
        shards, mesh=mesh, in_specs=placed, out_specs=P("tile", "src", None, None), check_vma=False
    )
```

```python
import functools
import math

import jax
import jax.numpy as jnp
from jax import lax
from jax.experimental import pallas as pl
from jax.experimental.pallas import tpu as pltpu
from jax.sharding import PartitionSpec as P

BY = 16
BZ = 64
SUB = 8
LANES = 128
ROWS = 32
DEPTH = 16
COMPS = 4
PIECES = 2
KK = 4

angular_rate = 9.0
MESH = pl.DeviceIdType.MESH

CHUNKS = (
    (8, 9, 9),
    (1, 8, 8),
    (1, 17, 17),
    (4, 18, 4),
    (4, 4, 18),
    (4, 0, 22),
    (4, 22, 0),
    (4, 26, 28),
    (2, 30, 26),
)
ARRIVALS = (((0, 1, 2), ()), ((3,), (4,)), ((5,), (6,)), ((7,), (8,)))
GROUPS = (
    ((2, 1), (2, 0)),
    ((1, 1), (3, 0)),
    ((3, 1), (1, 0)),
    ((4, 1), (4, 0)),
)


def sine_coefficients():
    import numpy as np

    n = 4
    k = np.arange(4000)
    r = 0.5 * np.cos((k + 0.5) * np.pi / 8000)
    powers = np.stack([r ** (2 * i + 1) for i in range(n)], axis=1)
    weight = 1.0 / np.sqrt(np.sin((k + 0.5) * np.pi / 8000) + 1e-3)
    target = np.sin(np.pi * r)
    for _ in range(60):
        got, *_rest = np.linalg.lstsq(powers * weight[:, None], target * weight, rcond=None)
        err = np.abs(powers @ got - target)
        weight = weight * (0.5 + 0.5 * err / err.max()) ** 0.5
        weight = weight / weight.max()
    return [float(np.float32(math.sqrt(2.0) * c)) for c in got]


def lane_masks(shape):
    lane = lax.broadcasted_iota(jnp.int32, shape, len(shape) - 1)
    sub = lax.broadcasted_iota(jnp.int32, shape, len(shape) - 2)
    z = lane & (BZ - 1)
    low = lane < BZ
    return z == 0, z == BZ - 1, low, low & (sub == 0), jnp.logical_not(low) & (sub == SUB - 1)


def kernel(
    coeffs,
    tables,
    weights_in,
    aperture_in,
    out,
    weights,
    aperture,
    small_sem,
    raw,
    send,
    recv,
    info_send,
    info_recv,
    splat,
    total_weight,
    fine,
    sib_send,
    sib_recv,
    far_send,
    far_recv,
    final,
    perm,
    load_sem,
    send_sem,
    recv_sem,
    info_ssem,
    info_rsem,
    sib_ssem,
    sib_rsem,
    far_ssem,
    far_rsem,
):
    a = lax.axis_index("src")
    t = lax.axis_index("tile")
    z, c = a // 2, a % 2
    tx, ty = t // 4, t % 4

    def owner_of(d):
        return ((tx + d // 4) % 4) * 4 + (ty + d % 4) % 4

    bar = pltpu.get_barrier_semaphore()

    def greet(d, carry):
        pl.semaphore_signal(bar, inc=1, device_id={"tile": owner_of(d), "src": a}, device_id_type=MESH)
        return carry

    lax.fori_loop(1, DEPTH, greet, 0)
    sibling = 2 * z + 1 - c
    pl.semaphore_signal(bar, inc=1, device_id={"src": sibling, "tile": t}, device_id_type=MESH)
    for m in range(3):
        far = 2 * ((z + 1 + m) % 4) + c
        pl.semaphore_signal(bar, inc=1, device_id={"src": far, "tile": t}, device_id_type=MESH)

    small = (
        pltpu.make_async_copy(weights_in, weights, small_sem.at[0]),
        pltpu.make_async_copy(aperture_in, aperture, small_sem.at[1]),
    )
    for copy in small:
        copy.start()

    def load(i):
        first = pl.multiple_of(((z + 1 + i) % 4) * SUB, SUB)
        return pltpu.make_async_copy(
            tables.at[0, :, pl.ds(first, SUB), :], raw.at[i], load_sem.at[i]
        )

    load(1).start()

    for copy in small:
        copy.wait()

    def fill_info(d, carry):
        first = 2 * owner_of(d)
        for j in range(2):
            w = jnp.full((SUB, LANES), weights[0, first + j], jnp.float32)
            live = jnp.full((SUB, LANES), aperture[0, first + j], jnp.int32)
            info_send[d, j] = w * live.astype(jnp.float32)
        return carry

    lax.fori_loop(0, DEPTH, fill_info, 0)

    scale = angular_rate / (2.0 * math.pi) / 64.0

    def pick(i):
        def one(d, carry):
            first = 2 * owner_of(d)
            second = jnp.full((SUB, LANES), aperture[0, first + 1], jnp.int32) == 1
            for k in range(8):
                lanes = pl.ds(k * LANES, LANES)
                chosen = jnp.where(second, raw[i, first + 1, :, lanes], raw[i, first, :, lanes])
                send[d, pl.ds((1 + 8 * i) * SUB + k, SUB, stride=SUB), :] = chosen * scale
            return carry

        lax.fori_loop(0, DEPTH, one, 0)

    load(1).wait()
    for i in (0, 2, 3):
        load(i).start()
    pick(1)

    pl.semaphore_wait(bar, DEPTH - 1 + 4)

    def rows_of(n):
        size, start1, start0 = CHUNKS[n]
        start = start0 + (start1 - start0) * c
        return pl.ds(pl.multiple_of(start * SUB, SUB), size * SUB)

    def send_info(d, carry):
        pltpu.make_async_remote_copy(
            info_send.at[d], info_recv.at[d], info_ssem, info_rsem,
            device_id={"tile": owner_of(d), "src": a}, device_id_type=MESH,
        ).start()
        return carry

    def send_chunk(n):
        rows = rows_of(n)

        def one(d, carry):
            pltpu.make_async_remote_copy(
                send.at[d, rows], recv.at[d, rows], send_sem.at[n], recv_sem.at[n],
                device_id={"tile": owner_of(d), "src": a}, device_id_type=MESH,
            ).start()
            return carry

        lax.fori_loop(1, DEPTH, one, 0)

    def own_chunk(n):
        rows = rows_of(n)
        recv[0, rows, :] = send[0, rows, :]

    lax.fori_loop(1, DEPTH, send_info, 0)
    send_chunk(0)
    load(0).wait()
    pick(0)
    send_chunk(1)
    load(2).wait()
    pick(2)
    for n in (2, 3, 4):
        send_chunk(n)
    load(3).wait()
    pick(3)

    def wrap(d, carry):
        send[d, pl.ds(0, SUB), :] = send[d, pl.ds(32 * SUB, SUB), :]
        return carry

    lax.fori_loop(0, DEPTH, wrap, 0)
    for n in range(5, len(CHUNKS)):
        send_chunk(n)
    for n in range(len(CHUNKS)):
        own_chunk(n)

    row = lax.broadcasted_iota(jnp.int32, (2 * LANES, 2 * LANES), 0)
    col = lax.broadcasted_iota(jnp.int32, (2 * LANES, 2 * LANES), 1)
    place = ((row // BZ) % 2) * LANES + 2 * (row % BZ) + row // LANES
    perm[...] = (col == place).astype(jnp.float32).astype(jnp.bfloat16)

    info_send_bytes = info_send.at[pl.ds(1, DEPTH - 1)]
    pltpu.make_async_copy(
        info_send_bytes, info_recv.at[pl.ds(1, DEPTH - 1)], info_rsem
    ).wait()
    splat[0] = info_send[0]
    splat[pl.ds(1, DEPTH - 1)] = info_recv[pl.ds(1, DEPTH - 1)]
    total_weight[...] = jnp.sum(splat[...], axis=0)

    def refine_rows(n):
        size, start1, start0 = CHUNKS[n]
        start = start0 + (start1 - start0) * c
        z_first, z_last, low, y_first, y_last = lane_masks((SUB, LANES))

        def one(i, carry):
            q = start + i
            for s in range(DEPTH):
                base = recv[s, pl.ds(pl.multiple_of(q * SUB, SUB), SUB), :]
                swap = pltpu.roll(base, BZ, 1)
                below = jnp.where(z_first, base, pltpu.roll(base, 1, 1))
                above = jnp.where(z_last, base, pltpu.roll(base, LANES - 1, 1))
                swap_below = jnp.where(z_first, swap, pltpu.roll(base, BZ + 1, 1))
                swap_above = jnp.where(z_last, swap, pltpu.roll(base, BZ - 1, 1))
                triple = 3.0 * base
                swap_triple = 3.0 * swap
                for pz in range(2):
                    v = triple + (above if pz else below)
                    w = swap_triple + (swap_above if pz else swap_below)
                    down = pltpu.roll(w, 1, 0)
                    up = pltpu.roll(w, SUB - 1, 0)
                    before = jnp.where(y_first, v, jnp.where(low, down, w))
                    after = jnp.where(y_last, v, jnp.where(low, w, up))
                    v3 = 3.0 * v
                    fine[q, s, pz] = v3 + before
                    fine[q, s, 2 + pz] = v3 + after
            return carry

        lax.fori_loop(0, size, one, 0)

    c0, c1, c2, c3 = coeffs

    def owner_place(m, who):
        (ahead1, half1), (ahead0, half0) = GROUPS[m]
        return ahead0 + (ahead1 - ahead0) * who, half0 + (half1 - half0) * who

    def piece_rows(p):
        return pl.ds(p * (8 // PIECES), 8 // PIECES)

    def partial_rows(m, who, target, p):
        ahead, half = owner_place(m, who)
        low_q = 8 * (ahead - 1) + 4 * half
        owner = 2 * ((z + ahead) % 4) + half
        at_first = (owner == 0).astype(jnp.int32)
        at_last = (owner == 7).astype(jnp.int32)
        per = KK // PIECES

        def one_row(kk, carry):
            k = (low_q + 1 + kk) % ROWS
            prev = (low_q + kk + at_first * (kk == 0).astype(jnp.int32)) % ROWS
            following = (low_q + 2 + kk - at_last * (kk == KK - 1).astype(jnp.int32)) % ROWS

            def some_sources(g, acc):
                acc = list(acc)
                for u in range(4):
                    s = g * 4 + u
                    f0 = splat[s, 0]
                    f1 = splat[s, 1]
                    for comp in range(COMPS):
                        center = 3.0 * fine[k, s, comp]
                        for par, other in enumerate((prev, following)):
                            phase = center + fine[other, s, comp]
                            r = phase - lax.round(phase, lax.RoundingMethod.TO_NEAREST_EVEN)
                            sq = r * r
                            root = r * (((c3 * sq + c2) * sq + c1) * sq + c0)
                            val = root * root
                            at = par * 8 + comp
                            acc[at] = acc[at] + f0 * val
                            acc[at + 4] = acc[at + 4] + f1 * val
                return tuple(acc)

            zero = jnp.zeros((SUB, LANES), jnp.float32)
            acc = lax.fori_loop(0, DEPTH // 4, some_sources, (zero,) * 16)
            for par in range(2):
                for tile in range(2):
                    for comp in range(COMPS):
                        target[2 * kk + par, tile, comp] = (
                            total_weight[tile] - acc[par * 8 + tile * 4 + comp]
                        )
            return carry

        lax.fori_loop(p * per, (p + 1) * per, one_row, 0)

    def to_sibling(m, p):
        return pltpu.make_async_remote_copy(
            sib_send.at[m, piece_rows(p)], sib_recv.at[m, piece_rows(p)],
            sib_ssem.at[m, p], sib_rsem.at[m, p],
            device_id={"src": sibling, "tile": t}, device_id_type=MESH,
        )

    def to_owner(m, p):
        ahead, half = owner_place(m, c)
        far = 2 * ((z + ahead) % 4) + half
        return pltpu.make_async_remote_copy(
            far_send.at[m, piece_rows(p)], far_recv.at[m, piece_rows(p)],
            far_ssem.at[m, p], far_rsem.at[m, p],
            device_id={"src": far, "tile": t}, device_id_type=MESH,
        )

    def wait_chunk(n):
        rows = rows_of(n)
        pltpu.make_async_copy(
            send.at[pl.ds(1, DEPTH - 1), rows], recv.at[pl.ds(1, DEPTH - 1), rows], recv_sem.at[n]
        ).wait()

    for m in range(4):
        for n in ARRIVALS[m][0]:
            wait_chunk(n)
        for n in ARRIVALS[m][0]:
            refine_rows(n)
        for p in range(PIECES):
            partial_rows(m, 1 - c, sib_send.at[m], p)
            to_sibling(m, p).start()
        for n in ARRIVALS[m][1]:
            wait_chunk(n)
            refine_rows(n)
        mine = far_send.at[m] if m < 3 else final
        for p in range(PIECES):
            partial_rows(m, c, mine, p)
            to_sibling(m, p).wait_recv()
            if m < 3:

                def add_sibling(x, carry):
                    far_send[m, x] = far_send[m, x] + sib_recv[m, x]
                    return carry

                lax.fori_loop(p * (8 // PIECES), (p + 1) * (8 // PIECES), add_sibling, 0)
                to_owner(m, p).start()

    for m in range(3):
        for p in range(PIECES):
            to_owner(m, p).wait_recv()

    for par in range(2):

        def finish(x, carry):
            for tile in range(2):
                for comp in range(2):
                    at = 2 * par + comp
                    got = final[x, tile, at] + sib_recv[3, x, tile, at]
                    for m in range(3):
                        got = got + far_recv[m, x, tile, at]
                    final[x, tile, at] = got
            return carry

        lax.fori_loop(0, 8, finish, 0)

    halves = [
        jnp.concatenate(
            [final[:, :, pl.ds(2 * par, 1)].reshape(16 * SUB, LANES),
             final[:, :, pl.ds(2 * par + 1, 1)].reshape(16 * SUB, LANES)], axis=1)
        for par in range(2)
    ]
    for par in range(2):
        value = halves[par]
        mixed = jnp.zeros((16 * SUB, 2 * LANES), jnp.float32)
        for _ in range(3):
            part = value.astype(jnp.bfloat16)
            value = value - part.astype(jnp.float32)
            mixed = mixed + jnp.dot(part, perm[...], preferred_element_type=jnp.float32)
        for x in range(8):
            for tile in range(2):
                at = (x * 2 + tile) * SUB
                for h in range(2):
                    out[tile, x, pl.ds(2 * h + par, SUB, stride=4), :] = (
                        mixed[at : at + SUB, h * LANES : (h + 1) * LANES]
                    )

    pltpu.make_async_copy(
        info_send_bytes, info_recv.at[pl.ds(1, DEPTH - 1)], info_ssem
    ).wait()
    for n in range(len(CHUNKS)):
        rows = rows_of(n)
        pltpu.make_async_copy(
            send.at[pl.ds(1, DEPTH - 1), rows], recv.at[pl.ds(1, DEPTH - 1), rows], send_sem.at[n]
        ).wait()
    for m in range(4):
        for p in range(PIECES):
            to_sibling(m, p).wait_send()
            if m < 3:
                to_owner(m, p).wait_send()


def shards(tables, weights, aperture):
    part = (8, 2, COMPS, SUB, LANES)
    vmem = pltpu.VMEM
    f32 = jnp.float32
    dma = pltpu.SemaphoreType.DMA
    return pl.pallas_call(
        functools.partial(kernel, sine_coefficients()),
        out_shape=jax.ShapeDtypeStruct((2, 8, 2 * BY, 2 * BZ), f32),
        in_specs=[
            pl.BlockSpec(memory_space=pl.ANY),
            pl.BlockSpec(memory_space=pl.ANY),
            pl.BlockSpec(memory_space=pl.ANY),
        ],
        out_specs=pl.BlockSpec(memory_space=pltpu.VMEM),
        scratch_shapes=[
            pltpu.SMEM((1, 32), f32),
            pltpu.SMEM((1, 32), jnp.int32),
            dma((2,)),
            vmem((4, 32, SUB, 1024), f32),
            vmem((DEPTH, 33 * SUB, LANES), f32),
            vmem((DEPTH, ROWS * SUB, LANES), f32),
            vmem((DEPTH, 2, SUB, LANES), f32),
            vmem((DEPTH, 2, SUB, LANES), f32),
            vmem((DEPTH, 2, SUB, LANES), f32),
            vmem((2, SUB, LANES), f32),
            vmem((ROWS, DEPTH, COMPS, SUB, LANES), f32),
            vmem((4,) + part, f32),
            vmem((4,) + part, f32),
            vmem((3,) + part, f32),
            vmem((3,) + part, f32),
            vmem(part, f32),
            vmem((2 * LANES, 2 * LANES), jnp.bfloat16),
            dma((4,)),
            dma((len(CHUNKS),)),
            dma((len(CHUNKS),)),
            dma,
            dma,
            dma((4, PIECES)),
            dma((4, PIECES)),
            dma((3, PIECES)),
            dma((3, PIECES)),
        ],
        compiler_params=pltpu.CompilerParams(
            collective_id=0, has_side_effects=True, vmem_limit_bytes=60 * 2**20
        ),
    )(tables, weights, aperture)


def solution(mesh):
    placed = (
        P(("src", "tile"), None, None, None),
        P(("src", "tile"), None),
        P(("src", "tile"), None),
    )
    return jax.shard_map(
        shards, mesh=mesh, in_specs=placed, out_specs=P("tile", "src", None, None), check_vma=False
    )
```

```python
import functools
import math

import jax
import jax.numpy as jnp
from jax import lax
from jax.experimental import pallas as pl
from jax.experimental.pallas import tpu as pltpu
from jax.sharding import PartitionSpec as P

BY = 16
BZ = 64
SUB = 8
LANES = 128
ROWS = 32
DEPTH = 16
COMPS = 4
PIECES = 2
KK = 4

angular_rate = 9.0
MESH = pl.DeviceIdType.MESH

CHUNKS = (
    (8, 9, 9),
    (1, 8, 8),
    (1, 17, 17),
    (4, 18, 4),
    (4, 4, 18),
    (4, 0, 22),
    (4, 22, 0),
    (4, 26, 28),
    (2, 30, 26),
)
ARRIVALS = (((0, 1, 2), ()), ((3,), (4,)), ((5,), (6,)), ((7,), (8,)))
GROUPS = (
    ((2, 1), (2, 0)),
    ((1, 1), (3, 0)),
    ((3, 1), (1, 0)),
    ((4, 1), (4, 0)),
)


def sine_coefficients():
    import numpy as np

    n = 4
    k = np.arange(4000)
    r = 0.5 * np.cos((k + 0.5) * np.pi / 8000)
    powers = np.stack([r ** (2 * i + 1) for i in range(n)], axis=1)
    weight = 1.0 / np.sqrt(np.sin((k + 0.5) * np.pi / 8000) + 1e-3)
    target = np.sin(np.pi * r)
    for _ in range(60):
        got, *_rest = np.linalg.lstsq(powers * weight[:, None], target * weight, rcond=None)
        err = np.abs(powers @ got - target)
        weight = weight * (0.5 + 0.5 * err / err.max()) ** 0.5
        weight = weight / weight.max()
    return [float(np.float32(math.sqrt(2.0) * c)) for c in got]


def lane_masks(shape):
    lane = lax.broadcasted_iota(jnp.int32, shape, len(shape) - 1)
    sub = lax.broadcasted_iota(jnp.int32, shape, len(shape) - 2)
    z = lane & (BZ - 1)
    low = lane < BZ
    return z == 0, z == BZ - 1, low, low & (sub == 0), jnp.logical_not(low) & (sub == SUB - 1)


def kernel(
    coeffs,
    tables,
    weights_in,
    aperture_in,
    out,
    weights,
    aperture,
    small_sem,
    raw,
    send,
    recv,
    info_send,
    info_recv,
    splat,
    total_weight,
    fine,
    sib_send,
    sib_recv,
    far_send,
    far_recv,
    final,
    perm,
    load_sem,
    send_sem,
    recv_sem,
    info_ssem,
    info_rsem,
    sib_ssem,
    sib_rsem,
    far_ssem,
    far_rsem,
):
    a = lax.axis_index("src")
    t = lax.axis_index("tile")
    z, c = a // 2, a % 2
    tx, ty = t // 4, t % 4

    def owner_of(d):
        return ((tx + d // 4) % 4) * 4 + (ty + d % 4) % 4

    bar = pltpu.get_barrier_semaphore()

    def greet(d, carry):
        pl.semaphore_signal(bar, inc=1, device_id={"tile": owner_of(d), "src": a}, device_id_type=MESH)
        return carry

    lax.fori_loop(1, DEPTH, greet, 0)
    sibling = 2 * z + 1 - c
    pl.semaphore_signal(bar, inc=1, device_id={"src": sibling, "tile": t}, device_id_type=MESH)
    for m in range(3):
        far = 2 * ((z + 1 + m) % 4) + c
        pl.semaphore_signal(bar, inc=1, device_id={"src": far, "tile": t}, device_id_type=MESH)

    small = (
        pltpu.make_async_copy(weights_in, weights, small_sem.at[0]),
        pltpu.make_async_copy(aperture_in, aperture, small_sem.at[1]),
    )
    for copy in small:
        copy.start()

    def load(i):
        first = pl.multiple_of(((z + 1 + i) % 4) * SUB, SUB)
        return pltpu.make_async_copy(
            tables.at[0, :, pl.ds(first, SUB), :], raw.at[i], load_sem.at[i]
        )

    load(1).start()

    for copy in small:
        copy.wait()

    def fill_info(d, carry):
        first = 2 * owner_of(d)
        for j in range(2):
            w = jnp.full((SUB, LANES), weights[0, first + j], jnp.float32)
            live = jnp.full((SUB, LANES), aperture[0, first + j], jnp.int32)
            info_send[d, j] = w * live.astype(jnp.float32)
        return carry

    lax.fori_loop(0, DEPTH, fill_info, 0)

    scale = angular_rate / (2.0 * math.pi) / 64.0

    def pick(i):
        def one(d, carry):
            first = 2 * owner_of(d)
            second = jnp.full((SUB, LANES), aperture[0, first + 1], jnp.int32) == 1
            for k in range(8):
                lanes = pl.ds(k * LANES, LANES)
                chosen = jnp.where(second, raw[i, first + 1, :, lanes], raw[i, first, :, lanes])
                send[d, pl.ds((1 + 8 * i) * SUB + k, SUB, stride=SUB), :] = chosen * scale
            return carry

        lax.fori_loop(0, DEPTH, one, 0)

    load(1).wait()
    for i in (0, 2, 3):
        load(i).start()
    pick(1)

    pl.semaphore_wait(bar, DEPTH - 1 + 4)

    def rows_of(n):
        size, start1, start0 = CHUNKS[n]
        start = start0 + (start1 - start0) * c
        return pl.ds(pl.multiple_of(start * SUB, SUB), size * SUB)

    def send_info(d, carry):
        pltpu.make_async_remote_copy(
            info_send.at[d], info_recv.at[d], info_ssem, info_rsem,
            device_id={"tile": owner_of(d), "src": a}, device_id_type=MESH,
        ).start()
        return carry

    def send_chunk(n):
        rows = rows_of(n)

        def one(d, carry):
            pltpu.make_async_remote_copy(
                send.at[d, rows], recv.at[d, rows], send_sem.at[n], recv_sem.at[n],
                device_id={"tile": owner_of(d), "src": a}, device_id_type=MESH,
            ).start()
            return carry

        lax.fori_loop(1, DEPTH, one, 0)

    def own_chunk(n):
        rows = rows_of(n)
        recv[0, rows, :] = send[0, rows, :]

    lax.fori_loop(1, DEPTH, send_info, 0)
    send_chunk(0)
    load(0).wait()
    pick(0)
    send_chunk(1)
    load(2).wait()
    pick(2)
    for n in (2, 3, 4):
        send_chunk(n)
    load(3).wait()
    pick(3)

    def wrap(d, carry):
        send[d, pl.ds(0, SUB), :] = send[d, pl.ds(32 * SUB, SUB), :]
        return carry

    lax.fori_loop(0, DEPTH, wrap, 0)
    for n in range(5, len(CHUNKS)):
        send_chunk(n)
    for n in range(len(CHUNKS)):
        own_chunk(n)

    row = lax.broadcasted_iota(jnp.int32, (2 * LANES, 2 * LANES), 0)
    col = lax.broadcasted_iota(jnp.int32, (2 * LANES, 2 * LANES), 1)
    place = ((row // BZ) % 2) * LANES + 2 * (row % BZ) + row // LANES
    perm[...] = (col == place).astype(jnp.float32).astype(jnp.bfloat16)

    info_send_bytes = info_send.at[pl.ds(1, DEPTH - 1)]
    pltpu.make_async_copy(
        info_send_bytes, info_recv.at[pl.ds(1, DEPTH - 1)], info_rsem
    ).wait()
    splat[0] = info_send[0]
    splat[pl.ds(1, DEPTH - 1)] = info_recv[pl.ds(1, DEPTH - 1)]
    total_weight[...] = jnp.sum(splat[...], axis=0)

    def refine_rows(n):
        size, start1, start0 = CHUNKS[n]
        start = start0 + (start1 - start0) * c
        z_first, z_last, low, y_first, y_last = lane_masks((SUB, LANES))

        def one(i, carry):
            q = start + i
            for s in range(DEPTH):
                base = recv[s, pl.ds(pl.multiple_of(q * SUB, SUB), SUB), :]
                swap = pltpu.roll(base, BZ, 1)
                below = jnp.where(z_first, base, pltpu.roll(base, 1, 1))
                above = jnp.where(z_last, base, pltpu.roll(base, LANES - 1, 1))
                swap_below = jnp.where(z_first, swap, pltpu.roll(base, BZ + 1, 1))
                swap_above = jnp.where(z_last, swap, pltpu.roll(base, BZ - 1, 1))
                triple = 3.0 * base
                swap_triple = 3.0 * swap
                for pz in range(2):
                    v = triple + (above if pz else below)
                    w = swap_triple + (swap_above if pz else swap_below)
                    down = pltpu.roll(w, 1, 0)
                    up = pltpu.roll(w, SUB - 1, 0)
                    before = jnp.where(y_first, v, jnp.where(low, down, w))
                    after = jnp.where(y_last, v, jnp.where(low, w, up))
                    v3 = 3.0 * v
                    fine[q, s, pz] = v3 + before
                    fine[q, s, 2 + pz] = v3 + after
            return carry

        lax.fori_loop(0, size, one, 0)

    c0, c1, c2, c3 = coeffs

    def owner_place(m, who):
        (ahead1, half1), (ahead0, half0) = GROUPS[m]
        return ahead0 + (ahead1 - ahead0) * who, half0 + (half1 - half0) * who

    def piece_rows(p):
        return pl.ds(p * (8 // PIECES), 8 // PIECES)

    def partial_rows(m, who, target, p):
        ahead, half = owner_place(m, who)
        low_q = 8 * (ahead - 1) + 4 * half
        owner = 2 * ((z + ahead) % 4) + half
        at_first = (owner == 0).astype(jnp.int32)
        at_last = (owner == 7).astype(jnp.int32)
        per = KK // PIECES

        def one_row(kk, carry):
            k = (low_q + 1 + kk) % ROWS
            prev = (low_q + kk + at_first * (kk == 0).astype(jnp.int32)) % ROWS
            following = (low_q + 2 + kk - at_last * (kk == KK - 1).astype(jnp.int32)) % ROWS

            def some_sources(g, acc):
                acc = list(acc)
                for u in range(4):
                    s = g * 4 + u
                    f0 = splat[s, 0]
                    f1 = splat[s, 1]
                    for comp in range(COMPS):
                        center = 3.0 * fine[k, s, comp]
                        for par, other in enumerate((prev, following)):
                            phase = center + fine[other, s, comp]
                            r = phase - lax.round(phase, lax.RoundingMethod.TO_NEAREST_EVEN)
                            sq = r * r
                            root = r * (((c3 * sq + c2) * sq + c1) * sq + c0)
                            val = root * root
                            at = par * 8 + comp
                            acc[at] = acc[at] + f0 * val
                            acc[at + 4] = acc[at + 4] + f1 * val
                return tuple(acc)

            zero = jnp.zeros((SUB, LANES), jnp.float32)
            acc = lax.fori_loop(0, DEPTH // 4, some_sources, (zero,) * 16)
            for par in range(2):
                for tile in range(2):
                    for comp in range(COMPS):
                        target[2 * kk + par, tile, comp] = (
                            total_weight[tile] - acc[par * 8 + tile * 4 + comp]
                        )
            return carry

        lax.fori_loop(p * per, (p + 1) * per, one_row, 0)

    def to_sibling(m, p):
        return pltpu.make_async_remote_copy(
            sib_send.at[m, piece_rows(p)], sib_recv.at[m, piece_rows(p)],
            sib_ssem.at[m, p], sib_rsem.at[m, p],
            device_id={"src": sibling, "tile": t}, device_id_type=MESH,
        )

    def to_owner(m, p):
        ahead, half = owner_place(m, c)
        far = 2 * ((z + ahead) % 4) + half
        return pltpu.make_async_remote_copy(
            far_send.at[m, piece_rows(p)], far_recv.at[m, piece_rows(p)],
            far_ssem.at[m, p], far_rsem.at[m, p],
            device_id={"src": far, "tile": t}, device_id_type=MESH,
        )

    def wait_chunk(n):
        rows = rows_of(n)
        pltpu.make_async_copy(
            send.at[pl.ds(1, DEPTH - 1), rows], recv.at[pl.ds(1, DEPTH - 1), rows], recv_sem.at[n]
        ).wait()

    for m in range(4):
        for n in ARRIVALS[m][0]:
            wait_chunk(n)
        for n in ARRIVALS[m][0]:
            refine_rows(n)
        for p in range(PIECES):
            partial_rows(m, 1 - c, sib_send.at[m], p)
            to_sibling(m, p).start()
        for n in ARRIVALS[m][1]:
            wait_chunk(n)
            refine_rows(n)
        mine = far_send.at[m] if m < 3 else final
        for p in range(PIECES):
            partial_rows(m, c, mine, p)
            to_sibling(m, p).wait_recv()
            if m < 3:

                def add_sibling(x, carry):
                    far_send[m, x] = far_send[m, x] + sib_recv[m, x]
                    return carry

                lax.fori_loop(p * (8 // PIECES), (p + 1) * (8 // PIECES), add_sibling, 0)
                to_owner(m, p).start()

    for m in range(3):
        for p in range(PIECES):
            to_owner(m, p).wait_recv()

    for par in range(2):

        def finish(x, carry):
            for tile in range(2):
                for comp in range(2):
                    at = 2 * par + comp
                    got = final[x, tile, at] + sib_recv[3, x, tile, at]
                    for m in range(3):
                        got = got + far_recv[m, x, tile, at]
                    final[x, tile, at] = got
            return carry

        lax.fori_loop(0, 8, finish, 0)

    halves = [
        jnp.concatenate(
            [final[:, :, pl.ds(2 * par, 1)].reshape(16 * SUB, LANES),
             final[:, :, pl.ds(2 * par + 1, 1)].reshape(16 * SUB, LANES)], axis=1)
        for par in range(2)
    ]
    for par in range(2):
        value = halves[par]
        mixed = jnp.zeros((16 * SUB, 2 * LANES), jnp.float32)
        for _ in range(3):
            part = value.astype(jnp.bfloat16)
            value = value - part.astype(jnp.float32)
            mixed = mixed + jnp.dot(part, perm[...], preferred_element_type=jnp.float32)
        for x in range(8):
            for tile in range(2):
                at = (x * 2 + tile) * SUB
                for h in range(2):
                    out[tile, x, pl.ds(2 * h + par, SUB, stride=4), :] = (
                        mixed[at : at + SUB, h * LANES : (h + 1) * LANES]
                    )

    pltpu.make_async_copy(
        info_send_bytes, info_recv.at[pl.ds(1, DEPTH - 1)], info_ssem
    ).wait()
    for n in range(len(CHUNKS)):
        rows = rows_of(n)
        pltpu.make_async_copy(
            send.at[pl.ds(1, DEPTH - 1), rows], recv.at[pl.ds(1, DEPTH - 1), rows], send_sem.at[n]
        ).wait()
    for m in range(4):
        for p in range(PIECES):
            to_sibling(m, p).wait_send()
            if m < 3:
                to_owner(m, p).wait_send()


def shards(tables, weights, aperture):
    part = (8, 2, COMPS, SUB, LANES)
    vmem = pltpu.VMEM
    f32 = jnp.float32
    dma = pltpu.SemaphoreType.DMA
    return pl.pallas_call(
        functools.partial(kernel, sine_coefficients()),
        out_shape=jax.ShapeDtypeStruct((2, 8, 2 * BY, 2 * BZ), f32),
        in_specs=[
            pl.BlockSpec(memory_space=pl.ANY),
            pl.BlockSpec(memory_space=pl.ANY),
            pl.BlockSpec(memory_space=pl.ANY),
        ],
        out_specs=pl.BlockSpec(memory_space=pltpu.VMEM),
        scratch_shapes=[
            pltpu.SMEM((1, 32), f32),
            pltpu.SMEM((1, 32), jnp.int32),
            dma((2,)),
            vmem((4, 32, SUB, 1024), f32),
            vmem((DEPTH, 33 * SUB, LANES), f32),
            vmem((DEPTH, ROWS * SUB, LANES), f32),
            vmem((DEPTH, 2, SUB, LANES), f32),
            vmem((DEPTH, 2, SUB, LANES), f32),
            vmem((DEPTH, 2, SUB, LANES), f32),
            vmem((2, SUB, LANES), f32),
            vmem((ROWS, DEPTH, COMPS, SUB, LANES), f32),
            vmem((4,) + part, f32),
            vmem((4,) + part, f32),
            vmem((3,) + part, f32),
            vmem((3,) + part, f32),
            vmem(part, f32),
            vmem((2 * LANES, 2 * LANES), jnp.bfloat16),
            dma((4,)),
            dma((len(CHUNKS),)),
            dma((len(CHUNKS),)),
            dma,
            dma,
            dma((4, PIECES)),
            dma((4, PIECES)),
            dma((3, PIECES)),
            dma((3, PIECES)),
        ],
        compiler_params=pltpu.CompilerParams(
            collective_id=0, has_side_effects=True, vmem_limit_bytes=51 * 2**20
        ),
    )(*(pltpu.with_memory_space_constraint(v, pltpu.HBM) for v in (tables, weights, aperture)))


def solution(mesh):
    placed = (
        P(("src", "tile"), None, None, None),
        P(("src", "tile"), None),
        P(("src", "tile"), None),
    )
    return jax.shard_map(
        shards, mesh=mesh, in_specs=placed, out_specs=P("tile", "src", None, None), check_vma=False
    )
```

```python
import functools
import math

import jax
import jax.numpy as jnp
from jax import lax
from jax.experimental import pallas as pl
from jax.experimental.pallas import tpu as pltpu
from jax.sharding import PartitionSpec as P

BY = 16
BZ = 64
SUB = 8
LANES = 128
ROWS = 32
DEPTH = 16
COMPS = 4
PIECES = 2
KK = 4

angular_rate = 9.0
MESH = pl.DeviceIdType.MESH

CHUNKS = (
    (8, 9, 9),
    (1, 8, 8),
    (1, 17, 17),
    (4, 18, 4),
    (4, 4, 18),
    (4, 0, 22),
    (4, 22, 0),
    (4, 26, 28),
    (2, 30, 26),
)
ARRIVALS = (((0, 1, 2), ()), ((3,), (4,)), ((5,), (6,)), ((7,), (8,)))
GROUPS = (
    ((2, 1), (2, 0)),
    ((1, 1), (3, 0)),
    ((3, 1), (1, 0)),
    ((4, 1), (4, 0)),
)


def sine_coefficients():
    import numpy as np

    n = 4
    k = np.arange(4000)
    r = 0.5 * np.cos((k + 0.5) * np.pi / 8000)
    powers = np.stack([r ** (2 * i + 1) for i in range(n)], axis=1)
    weight = 1.0 / np.sqrt(np.sin((k + 0.5) * np.pi / 8000) + 1e-3)
    target = np.sin(np.pi * r)
    for _ in range(60):
        got, *_rest = np.linalg.lstsq(powers * weight[:, None], target * weight, rcond=None)
        err = np.abs(powers @ got - target)
        weight = weight * (0.5 + 0.5 * err / err.max()) ** 0.5
        weight = weight / weight.max()
    return [float(np.float32(math.sqrt(2.0) * c)) for c in got]


def lane_masks(shape):
    lane = lax.broadcasted_iota(jnp.int32, shape, len(shape) - 1)
    sub = lax.broadcasted_iota(jnp.int32, shape, len(shape) - 2)
    z = lane & (BZ - 1)
    low = lane < BZ
    return z == 0, z == BZ - 1, low, low & (sub == 0), jnp.logical_not(low) & (sub == SUB - 1)


def kernel(
    coeffs,
    tables,
    weights_in,
    aperture_in,
    out,
    weights,
    aperture,
    small_sem,
    raw,
    send,
    recv,
    info_send,
    info_recv,
    splat,
    total_weight,
    fine,
    sib_send,
    sib_recv,
    far_send,
    far_recv,
    final,
    perm,
    load_sem,
    send_sem,
    recv_sem,
    info_ssem,
    info_rsem,
    sib_ssem,
    sib_rsem,
    far_ssem,
    far_rsem,
):
    a = lax.axis_index("src")
    t = lax.axis_index("tile")
    z, c = a // 2, a % 2
    tx, ty = t // 4, t % 4

    def owner_of(d):
        return ((tx + d // 4) % 4) * 4 + (ty + d % 4) % 4

    bar = pltpu.get_barrier_semaphore()

    def greet(d, carry):
        pl.semaphore_signal(bar, inc=1, device_id={"tile": owner_of(d), "src": a}, device_id_type=MESH)
        return carry

    lax.fori_loop(1, DEPTH, greet, 0)
    sibling = 2 * z + 1 - c
    pl.semaphore_signal(bar, inc=1, device_id={"src": sibling, "tile": t}, device_id_type=MESH)
    for m in range(3):
        far = 2 * ((z + 1 + m) % 4) + c
        pl.semaphore_signal(bar, inc=1, device_id={"src": far, "tile": t}, device_id_type=MESH)

    small = (
        pltpu.make_async_copy(weights_in, weights, small_sem.at[0]),
        pltpu.make_async_copy(aperture_in, aperture, small_sem.at[1]),
    )
    for copy in small:
        copy.start()

    def load(i):
        first = pl.multiple_of(((z + 1 + i) % 4) * SUB, SUB)
        return pltpu.make_async_copy(
            tables.at[0, :, pl.ds(first, SUB), :], raw.at[i], load_sem.at[i]
        )

    load(1).start()

    for copy in small:
        copy.wait()

    def fill_info(d, carry):
        first = 2 * owner_of(d)
        for j in range(2):
            w = jnp.full((SUB, LANES), weights[0, first + j], jnp.float32)
            live = jnp.full((SUB, LANES), aperture[0, first + j], jnp.int32)
            info_send[d, pl.ds(j, 1), :] = (w * live.astype(jnp.float32))[0:1]
        return carry

    lax.fori_loop(0, DEPTH, fill_info, 0)

    scale = angular_rate / (2.0 * math.pi) / 64.0

    def pick(i):
        def one(d, carry):
            first = 2 * owner_of(d)
            second = jnp.full((SUB, LANES), aperture[0, first + 1], jnp.int32) == 1
            for k in range(8):
                lanes = pl.ds(k * LANES, LANES)
                chosen = jnp.where(second, raw[i, first + 1, :, lanes], raw[i, first, :, lanes])
                send[d, pl.ds((1 + 8 * i) * SUB + k, SUB, stride=SUB), :] = chosen * scale
            return carry

        lax.fori_loop(0, DEPTH, one, 0)

    load(1).wait()
    for i in (0, 2, 3):
        load(i).start()
    pick(1)

    pl.semaphore_wait(bar, DEPTH - 1 + 4)

    def rows_of(n):
        size, start1, start0 = CHUNKS[n]
        start = start0 + (start1 - start0) * c
        return pl.ds(pl.multiple_of(start * SUB, SUB), size * SUB)

    def send_info(d, carry):
        pltpu.make_async_remote_copy(
            info_send.at[d, pl.ds(0, 2)], info_recv.at[d, pl.ds(0, 2)], info_ssem, info_rsem,
            device_id={"tile": owner_of(d), "src": a}, device_id_type=MESH,
        ).start()
        return carry

    def send_chunk(n):
        rows = rows_of(n)

        def one(d, carry):
            pltpu.make_async_remote_copy(
                send.at[d, rows], recv.at[d, rows], send_sem.at[n], recv_sem.at[n],
                device_id={"tile": owner_of(d), "src": a}, device_id_type=MESH,
            ).start()
            return carry

        lax.fori_loop(1, DEPTH, one, 0)

    def own_chunk(n):
        rows = rows_of(n)
        recv[0, rows, :] = send[0, rows, :]

    send_chunk(0)
    lax.fori_loop(1, DEPTH, send_info, 0)
    load(0).wait()
    pick(0)
    send_chunk(1)
    load(2).wait()
    pick(2)
    for n in (2, 3, 4):
        send_chunk(n)
    load(3).wait()
    pick(3)

    def wrap(d, carry):
        send[d, pl.ds(0, SUB), :] = send[d, pl.ds(32 * SUB, SUB), :]
        return carry

    lax.fori_loop(0, DEPTH, wrap, 0)
    for n in range(5, len(CHUNKS)):
        send_chunk(n)
    for n in range(len(CHUNKS)):
        own_chunk(n)

    row = lax.broadcasted_iota(jnp.int32, (2 * LANES, 2 * LANES), 0)
    col = lax.broadcasted_iota(jnp.int32, (2 * LANES, 2 * LANES), 1)
    place = ((row // BZ) % 2) * LANES + 2 * (row % BZ) + row // LANES
    perm[...] = (col == place).astype(jnp.float32).astype(jnp.bfloat16)

    info_out = info_send.at[pl.ds(1, DEPTH - 1), pl.ds(0, 2)]
    info_in = info_recv.at[pl.ds(1, DEPTH - 1), pl.ds(0, 2)]
    pltpu.make_async_copy(info_out, info_in, info_rsem).wait()
    for s in range(DEPTH):
        origin = info_recv if s else info_send
        for j in range(2):
            splat[s, j] = jnp.broadcast_to(origin[s, pl.ds(j, 1), :], (SUB, LANES))
    total_weight[...] = jnp.sum(splat[...], axis=0)

    def refine_rows(n):
        size, start1, start0 = CHUNKS[n]
        start = start0 + (start1 - start0) * c
        z_first, z_last, low, y_first, y_last = lane_masks((SUB, LANES))

        def one(i, carry):
            q = start + i
            for s in range(DEPTH):
                base = recv[s, pl.ds(pl.multiple_of(q * SUB, SUB), SUB), :]
                swap = pltpu.roll(base, BZ, 1)
                below = jnp.where(z_first, base, pltpu.roll(base, 1, 1))
                above = jnp.where(z_last, base, pltpu.roll(base, LANES - 1, 1))
                swap_below = jnp.where(z_first, swap, pltpu.roll(base, BZ + 1, 1))
                swap_above = jnp.where(z_last, swap, pltpu.roll(base, BZ - 1, 1))
                triple = 3.0 * base
                swap_triple = 3.0 * swap
                for pz in range(2):
                    v = triple + (above if pz else below)
                    w = swap_triple + (swap_above if pz else swap_below)
                    down = pltpu.roll(w, 1, 0)
                    up = pltpu.roll(w, SUB - 1, 0)
                    before = jnp.where(y_first, v, jnp.where(low, down, w))
                    after = jnp.where(y_last, v, jnp.where(low, w, up))
                    v3 = 3.0 * v
                    fine[q, s, pz] = v3 + before
                    fine[q, s, 2 + pz] = v3 + after
            return carry

        lax.fori_loop(0, size, one, 0)

    c0, c1, c2, c3 = coeffs

    def owner_place(m, who):
        (ahead1, half1), (ahead0, half0) = GROUPS[m]
        return ahead0 + (ahead1 - ahead0) * who, half0 + (half1 - half0) * who

    def piece_rows(p):
        return pl.ds(p * (8 // PIECES), 8 // PIECES)

    def partial_rows(m, who, target, p):
        ahead, half = owner_place(m, who)
        low_q = 8 * (ahead - 1) + 4 * half
        owner = 2 * ((z + ahead) % 4) + half
        at_first = (owner == 0).astype(jnp.int32)
        at_last = (owner == 7).astype(jnp.int32)
        per = KK // PIECES

        def one_row(kk, carry):
            k = (low_q + 1 + kk) % ROWS
            prev = (low_q + kk + at_first * (kk == 0).astype(jnp.int32)) % ROWS
            following = (low_q + 2 + kk - at_last * (kk == KK - 1).astype(jnp.int32)) % ROWS

            def some_sources(g, acc):
                acc = list(acc)
                for u in range(4):
                    s = g * 4 + u
                    f0 = splat[s, 0]
                    f1 = splat[s, 1]
                    for comp in range(COMPS):
                        center = 3.0 * fine[k, s, comp]
                        for par, other in enumerate((prev, following)):
                            phase = center + fine[other, s, comp]
                            r = phase - lax.round(phase, lax.RoundingMethod.TO_NEAREST_EVEN)
                            sq = r * r
                            root = r * (((c3 * sq + c2) * sq + c1) * sq + c0)
                            val = root * root
                            at = par * 8 + comp
                            acc[at] = acc[at] + f0 * val
                            acc[at + 4] = acc[at + 4] + f1 * val
                return tuple(acc)

            zero = jnp.zeros((SUB, LANES), jnp.float32)
            acc = lax.fori_loop(0, DEPTH // 4, some_sources, (zero,) * 16)
            for par in range(2):
                for tile in range(2):
                    for comp in range(COMPS):
                        target[2 * kk + par, tile, comp] = (
                            total_weight[tile] - acc[par * 8 + tile * 4 + comp]
                        )
            return carry

        lax.fori_loop(p * per, (p + 1) * per, one_row, 0)

    def to_sibling(m, p):
        return pltpu.make_async_remote_copy(
            sib_send.at[m, piece_rows(p)], sib_recv.at[m, piece_rows(p)],
            sib_ssem.at[m, p], sib_rsem.at[m, p],
            device_id={"src": sibling, "tile": t}, device_id_type=MESH,
        )

    def to_owner(m, p):
        ahead, half = owner_place(m, c)
        far = 2 * ((z + ahead) % 4) + half
        return pltpu.make_async_remote_copy(
            far_send.at[m, piece_rows(p)], far_recv.at[m, piece_rows(p)],
            far_ssem.at[m, p], far_rsem.at[m, p],
            device_id={"src": far, "tile": t}, device_id_type=MESH,
        )

    def wait_chunk(n):
        rows = rows_of(n)
        pltpu.make_async_copy(
            send.at[pl.ds(1, DEPTH - 1), rows], recv.at[pl.ds(1, DEPTH - 1), rows], recv_sem.at[n]
        ).wait()

    for m in range(4):
        for n in ARRIVALS[m][0]:
            wait_chunk(n)
        for n in ARRIVALS[m][0]:
            refine_rows(n)
        for p in range(PIECES):
            partial_rows(m, 1 - c, sib_send.at[m], p)
            to_sibling(m, p).start()
        for n in ARRIVALS[m][1]:
            wait_chunk(n)
            refine_rows(n)
        mine = far_send.at[m] if m < 3 else final
        if m == 3:
            for k in range(2):
                for p in range(PIECES):
                    to_owner(k, p).wait_recv()

            def add_far(x, carry):
                far_recv[0, x] = far_recv[0, x] + far_recv[1, x]
                return carry

            lax.fori_loop(0, 8, add_far, 0)
        for p in range(PIECES):
            partial_rows(m, c, mine, p)
            to_sibling(m, p).wait_recv()
            if m < 3:

                def add_sibling(x, carry):
                    far_send[m, x] = far_send[m, x] + sib_recv[m, x]
                    return carry

                lax.fori_loop(p * (8 // PIECES), (p + 1) * (8 // PIECES), add_sibling, 0)
                to_owner(m, p).start()

    for p in range(PIECES):
        to_owner(2, p).wait_recv()

    for par in range(2):

        def finish(x, carry):
            for tile in range(2):
                for comp in range(2):
                    at = 2 * par + comp
                    got = final[x, tile, at] + sib_recv[3, x, tile, at]
                    got = got + far_recv[0, x, tile, at] + far_recv[2, x, tile, at]
                    final[x, tile, at] = got
            return carry

        lax.fori_loop(0, 8, finish, 0)

    halves = [
        jnp.concatenate(
            [final[:, :, pl.ds(2 * par, 1)].reshape(16 * SUB, LANES),
             final[:, :, pl.ds(2 * par + 1, 1)].reshape(16 * SUB, LANES)], axis=1)
        for par in range(2)
    ]
    for par in range(2):
        value = halves[par]
        mixed = jnp.zeros((16 * SUB, 2 * LANES), jnp.float32)
        for _ in range(2):
            part = value.astype(jnp.bfloat16)
            value = value - part.astype(jnp.float32)
            mixed = mixed + jnp.dot(part, perm[...], preferred_element_type=jnp.float32)
        for x in range(8):
            for tile in range(2):
                at = (x * 2 + tile) * SUB
                for h in range(2):
                    out[tile, x, pl.ds(2 * h + par, SUB, stride=4), :] = (
                        mixed[at : at + SUB, h * LANES : (h + 1) * LANES]
                    )

    pltpu.make_async_copy(info_out, info_in, info_ssem).wait()
    for n in range(len(CHUNKS)):
        rows = rows_of(n)
        pltpu.make_async_copy(
            send.at[pl.ds(1, DEPTH - 1), rows], recv.at[pl.ds(1, DEPTH - 1), rows], send_sem.at[n]
        ).wait()
    for m in range(4):
        for p in range(PIECES):
            to_sibling(m, p).wait_send()
            if m < 3:
                to_owner(m, p).wait_send()


def shards(tables, weights, aperture):
    part = (8, 2, COMPS, SUB, LANES)
    vmem = pltpu.VMEM
    f32 = jnp.float32
    dma = pltpu.SemaphoreType.DMA
    return pl.pallas_call(
        functools.partial(kernel, sine_coefficients()),
        out_shape=jax.ShapeDtypeStruct((2, 8, 2 * BY, 2 * BZ), f32),
        in_specs=[
            pl.BlockSpec(memory_space=pl.ANY),
            pl.BlockSpec(memory_space=pl.ANY),
            pl.BlockSpec(memory_space=pl.ANY),
        ],
        out_specs=pl.BlockSpec(memory_space=pltpu.VMEM),
        scratch_shapes=[
            pltpu.SMEM((1, 32), f32),
            pltpu.SMEM((1, 32), jnp.int32),
            dma((2,)),
            vmem((4, 32, SUB, 1024), f32),
            vmem((DEPTH, 33 * SUB, LANES), f32),
            vmem((DEPTH, ROWS * SUB, LANES), f32),
            vmem((DEPTH, SUB, LANES), f32),
            vmem((DEPTH, SUB, LANES), f32),
            vmem((DEPTH, 2, SUB, LANES), f32),
            vmem((2, SUB, LANES), f32),
            vmem((ROWS, DEPTH, COMPS, SUB, LANES), f32),
            vmem((4,) + part, f32),
            vmem((4,) + part, f32),
            vmem((3,) + part, f32),
            vmem((3,) + part, f32),
            vmem(part, f32),
            vmem((2 * LANES, 2 * LANES), jnp.bfloat16),
            dma((4,)),
            dma((len(CHUNKS),)),
            dma((len(CHUNKS),)),
            dma,
            dma,
            dma((4, PIECES)),
            dma((4, PIECES)),
            dma((3, PIECES)),
            dma((3, PIECES)),
        ],
        compiler_params=pltpu.CompilerParams(
            collective_id=0, has_side_effects=True, vmem_limit_bytes=51 * 2**20
        ),
    )(*(pltpu.with_memory_space_constraint(v, pltpu.HBM) for v in (tables, weights, aperture)))


def solution(mesh):
    placed = (
        P(("src", "tile"), None, None, None),
        P(("src", "tile"), None),
        P(("src", "tile"), None),
    )
    return jax.shard_map(
        shards, mesh=mesh, in_specs=placed, out_specs=P("tile", "src", None, None), check_vma=False
    )
```
